256 devices in a mesh: band: 4 (over x_lo, core), fft: 64 (over y, z, x_hi).
Axes of the slice: x: 4 (x_hi: 2, x_lo: 2; x = x_hi * 2 + x_lo), y: 4, z: 8, core: 2. Of those that a mesh axis runs over, the one named last changes fastest.
Arguments:
- orbitals: bfloat16 [16, 2, 262144], P('band', None, 'fft'), may hold values from -6 to 6
- sphere_slot: int32 [262144], P('fft'), may hold values from 0 to 24575, as said below
- stick_column: int32 [8192], P('fft'), may hold values from 0 to 36863, as said below
- potential: float32 [192, 192, 192], P('fft'), may hold values from -3 to 3
- subspace: bfloat16 [64, 2, 262144], P('band', None, 'fft'), may hold values from -0.0234375 to 0.0234375
- previous: bfloat16 [16, 2, 262144], P('band', None, 'fft'), may hold values from -6 to 6
Outputs:
- applied: bfloat16 [16, 2, 262144], P('band', None, 'fft')
- intersection: float32 [2, 64, 16], P(None, 'fft', 'band')
The draws below stay inside these ranges and needn't reach their ends.
Inputs may be any that keep to these rules, and one draw needn't show every extreme that they name: `sphere_slot`: within each aligned block of 4096 entries the values are distinct. `stick_column`: aligned block d of 128 entries holds distinct columns x * 192 + y with d * 3 <= x < (d + 1) * 3.
All inputs are finite; a program needn't handle non-finite values.
Results may differ from the reference program's by a relative error of at most 0.012.
Values may be sent and summed in bfloat16 or wider, within the bound.
No kernel may reach another device: no remote copies, remote signals or barrier semaphores. Data moves between devices by JAX's collectives and lax.ppermute only.
A program may use at most 64 MiB of HBM per device.

```python
import jax
import jax.numpy as jnp
from jax import lax

NG = 192
STK = 128
NPW_DEV = 4096
SUBB = 64
BANDS = 16
STICKS = 8192
NPW_TOT = 262144


def draw_sphere_slot(key, part):
    blocks = NPW_TOT // NPW_DEV
    keys = jax.random.split(jax.random.fold_in(key, 11), blocks)

    def one_block(block_key):
        return jax.random.permutation(block_key, NG * STK)[:NPW_DEV].astype(jnp.int32)
    return jax.vmap(one_block)(keys).reshape(-1).astype(jnp.int32)


def draw_stick_column(key, part):
    blocks = STICKS // STK
    slab_cells = NG // blocks * NG
    keys = jax.random.split(jax.random.fold_in(key, 23), blocks)

    def one_block(block_key, owner):
        return jax.random.permutation(block_key, slab_cells)[:STK].astype(jnp.int32) + owner * slab_cells
    owners = jnp.arange(blocks, dtype=jnp.int32)
    return jax.vmap(one_block)(keys, owners).reshape(-1).astype(jnp.int32)


def strengthened(result, rng, source, target, shards_of, factor):
    def block_of(axis_at):
        return (jnp.arange(result.shape[axis_at]) // (result.shape[axis_at] // shards_of)).reshape((-1,) + (1,) * (result.ndim - 1 - axis_at))

    first = jax.random.permutation(rng, shards_of)[block_of(target)]
    other_side = (block_of(target) + shards_of // 2) % shards_of
    return jnp.where((block_of(source) == first) | (block_of(source) == other_side), factor * result, result)


def level_of(stream_key, shape, cuts, low, high):
    factor_of, own = 1.0, jax.random.fold_in(stream_key, 6)
    for position, blocks in cuts:
        steps = jnp.exp(jax.random.uniform(jax.random.fold_in(own, position), (blocks,), jnp.float32, low / len(cuts), high / len(cuts)))
        factor_of = factor_of * jnp.repeat(steps, shape[position] // blocks).reshape([-1 if axis == position else 1 for axis in range(len(shape))])
    return factor_of


def scatter_about(own_key, extent, scale, reach, pieces=(), held_as=jnp.bfloat16):
    array = scale * jax.random.normal(own_key, extent, jnp.float32)
    if pieces:
        array = array * level_of(own_key, extent, pieces, -0.22, 0.18)
    return jnp.clip(array, -reach, reach).astype(held_as)


def bell_draw_with(rng, dims, scale, reach, cuts, heavy, kind=jnp.bfloat16):
    values = scale * jax.random.normal(rng, dims, jnp.float32)
    if cuts:
        values = values * level_of(rng, dims, cuts, -0.22, 0.18)
    return jnp.clip(strengthened(values, jax.random.fold_in(rng, 3), *heavy), -reach, reach).astype(kind)


def setup_inputs(seed: int = 0) -> dict:
    seeds = jax.random.split(jax.random.key(seed), 7)
    return {
        "orbitals": scatter_about(seeds[0], (BANDS, 2, NPW_TOT), 1.0, 6.0, ((0, 4), (2, 64))),
        "sphere_slot": draw_sphere_slot(jax.random.fold_in(seeds[6], 71), 0),
        "stick_column": draw_stick_column(jax.random.fold_in(seeds[6], 71), 0),
        "potential": jnp.clip(jax.random.uniform(seeds[3], (NG, NG, NG), jnp.float32, -3.0, 3.0) * level_of(seeds[3], (NG, NG, NG), ((0, 64),), -0.4, 0.0), -3.0, 3.0),
        "subspace": bell_draw_with(seeds[4], (SUBB, 2, NPW_TOT), (2 * NPW_TOT) ** -0.5, 0.0234375, ((0, 4), (2, 64)), (2, 0, 64, 4.0)),
        "previous": scatter_about(seeds[5], (BANDS, 2, NPW_TOT), 1.0, 6.0, ((0, 4), (2, 64))),
    }


def frequency(values, grid_size):
    return jnp.where(values >= grid_size // 2, values - grid_size, values).astype(jnp.float32)


def rounded(values):
    real_part = lax.optimization_barrier(jnp.real(values).astype(jnp.bfloat16)).astype(jnp.float32)
    imag_part = lax.optimization_barrier(jnp.imag(values).astype(jnp.bfloat16)).astype(jnp.float32)
    return lax.complex(real_part, imag_part)


def reference(orbitals, sphere_slot, stick_column, potential, subspace, previous):
    owner = jnp.arange(NPW_TOT, dtype=jnp.int32) // NPW_DEV
    plane_index = (sphere_slot // STK).astype(jnp.int32)
    column = stick_column[(owner * STK + sphere_slot % STK).astype(jnp.int32)]
    cell = (plane_index * (NG * NG) + column).astype(jnp.int32)
    freq_z = frequency(plane_index, NG)
    freq_x = frequency(column // NG, NG)
    freq_y = frequency(column % NG, NG)
    kinetic = (freq_z * freq_z + freq_x * freq_x + freq_y * freq_y) * (2.0 / (NG * NG))

    def one_band(coeffs):
        real_in = coeffs[0].astype(jnp.float32)
        imag_in = coeffs[1].astype(jnp.float32)
        empty = jnp.zeros((NG * NG * NG,), jnp.float32)
        grid = lax.complex(empty.at[cell].set(real_in), empty.at[cell].set(imag_in)).reshape(NG, NG, NG)
        grid = rounded(jnp.fft.ifft(grid, axis=0, norm="forward"))
        grid = rounded(jnp.fft.ifft(grid, axis=2, norm="forward"))
        grid = rounded(jnp.fft.ifft(grid, axis=1, norm="forward") * potential)
        grid = rounded(jnp.fft.fft(grid, axis=1, norm="forward"))
        grid = rounded(jnp.fft.fft(grid, axis=2, norm="forward"))
        grid = jnp.fft.fft(grid, axis=0, norm="forward")
        values = grid.reshape(-1)[cell]
        applied_real = jnp.real(values) + kinetic * real_in
        applied_imag = jnp.imag(values) + kinetic * imag_in
        return jnp.stack([applied_real, applied_imag]).astype(jnp.bfloat16)

    applied = lax.map(one_band, orbitals)
    sub_real = subspace[:, 0]
    sub_imag = subspace[:, 1]
    prev_real = previous[:, 0]
    prev_imag = previous[:, 1]
    over_real = jnp.dot(sub_real, prev_real.T, preferred_element_type=jnp.float32) + jnp.dot(sub_imag, prev_imag.T, preferred_element_type=jnp.float32)
    over_imag = jnp.dot(sub_real, prev_imag.T, preferred_element_type=jnp.float32) - jnp.dot(sub_imag, prev_real.T, preferred_element_type=jnp.float32)
    return applied, jnp.stack([over_real, over_imag])
```

```python
import functools
import math

import jax
import jax.numpy as jnp
import numpy as np
from jax import lax
from jax.experimental import pallas as pl
from jax.experimental.pallas import tpu as pltpu
from jax.sharding import PartitionSpec as P

BF = jnp.bfloat16
F32 = jnp.float32
N = 192
OWN = 64
DEP = N // OWN
STK = 128
W = 256
EXT = 8
NT = (((1,), (1,)), ((), ()))
TN = (((0,), (0,)), ((), ()))


def dot(a, b, dims=(((1,), (0,)), ((), ()))):
    return lax.dot_general(a, b, dims, preferred_element_type=F32)


@functools.cache
def tables():
    def trig(rows, cols, scale):
        angle = (np.outer(rows, cols) % N) * (2.0 * math.pi / N)
        return np.cos(angle) * scale, np.sin(angle) * scale

    nat = np.arange(N)
    dealt = (np.arange(DEP)[:, None] + DEP * np.arange(OWN)[None, :]).reshape(-1)

    def wide(a, rows, cols):
        out = np.zeros((rows, cols))
        out[: a.shape[0], : a.shape[1]] = a
        return out

    def left(rows, cols, scale, sign, width):
        c, s = trig(rows, cols, scale)
        c, s = wide(c, N, width), wide(s * sign, N, width)
        return np.block([[c, -s], [s, c]])

    def right(rows, cols, scale, sign, height, width):
        c, s = trig(rows, cols, scale)
        c, s = wide(c, height, width), wide(s * sign, height, width)
        return np.block([[c, s], [-s, c]])

    inv = 1.0 / N
    out = {
        "zf": left(dealt, nat, 1.0, 1.0, W),
        "yf": right(nat, nat, 1.0, 1.0, W, W),
        "xf": left(nat, dealt, 1.0, 1.0, N),
        "xi": left(dealt, nat, inv, -1.0, N),
        "yi": right(nat, nat, inv, -1.0, W, W),
        "zi": right(dealt, nat, inv, -1.0, N, W),
    }
    return {k: v.astype(np.float32).astype(BF) for k, v in out.items()}


def iota(shape, dim):
    return lax.broadcasted_iota(jnp.int32, shape, dim)


def column_coords(col):
    c = col.astype(F32)
    x = jnp.floor((c + 0.5) * (1.0 / N))
    return x, c - x * N


def pack_kernel(orb_ref, slot_ref, col_ref, zf_ref, out_ref, a_scr, b_scr):
    npw = slot_ref.shape[1]
    slot = slot_ref[...]
    low = slot & 63
    high = ((slot >> 6) & 1) * W + (slot >> 7)
    half = 1024
    for i in range(0, npw, half):
        cut = slice(i, i + half)
        a_scr[:, cut] = jnp.where(iota((2 * W, half), 0) == high[:, cut], 1.0, 0.0).astype(BF)
        hit = iota((64, half), 0) == low[:, cut]
        for j in range(8):
            row = orb_ref[j : j + 1, cut].astype(F32)
            b_scr[64 * j : 64 * (j + 1), cut] = jnp.where(hit, row, 0.0).astype(BF)
    grid = dot(b_scr[...], a_scr[...], NT).astype(BF)
    rows = []
    for b in range(4):
        for h in range(2):
            rows.append(
                jnp.concatenate(
                    [grid[64 * (2 * b + p) : 64 * (2 * b + p + 1), W * h : W * (h + 1)] for p in range(2)],
                    axis=1,
                )
            )
    stick = jnp.concatenate(rows, axis=0)
    wave = dot(zf_ref[...], stick, NT)
    x, y = column_coords(col_ref[...])
    xl = x - DEP * jnp.floor((x + 0.5) * (1.0 / DEP))
    ext = jnp.where(iota((EXT, STK), 0) == 0, xl, jnp.where(iota((EXT, STK), 0) == 1, y, 0.0))
    parts = [jnp.broadcast_to(ext[e : e + 1, :], (OWN, STK)) for e in range(EXT)]
    for r in range(DEP):
        for b in range(4):
            for p in range(2):
                base = p * N + r * OWN
                parts.append(wave[base : base + OWN, STK * b : STK * (b + 1)])
    out_ref[...] = jnp.swapaxes(jnp.stack(parts, axis=0), 0, 1).astype(BF)


def plane_kernel(
    in_ref, ext_ref, pot_ref, yf_ref, xf_ref, xi_ref, yi_ref, out_ref, rt_scr, oh_scr, lhs_scr, f_scr, pot_scr
):
    rows = 8 * DEP
    rt_scr[...] = jnp.swapaxes(in_ref[...].astype(F32), 0, 1)
    pot_scr[...] = jnp.zeros(pot_scr.shape, F32)
    pot_scr[:, :, :N] = pot_ref[...]
    sub = iota((8, STK), 0)

    def scatter(g, carry):
        at = pl.multiple_of(g * 8, 8)
        xl = rt_scr[0, pl.ds(at, 8), :]
        y = rt_scr[1, pl.ds(at, 8), :].astype(jnp.int32)
        for d in range(8):
            oh_scr[g, :, STK * d : STK * (d + 1)] = jnp.where(iota((W, STK), 0) == y[d : d + 1, :], 1.0, 0.0).astype(BF)
        for k in range(DEP):
            for row in range(0, rows, 2):
                v = [jnp.where(xl == k, rt_scr[EXT + row + t, pl.ds(at, 8), :], 0.0) for t in range(2)]
                for d in range(8):
                    block = jnp.concatenate([jnp.where(sub == d, u, 0.0) for u in v], axis=0).astype(BF)
                    base = (k * rows + row) * 8
                    lhs_scr[base : base + 16, STK * d : STK * (d + 1)] = block
        res = dot(lhs_scr[...], oh_scr[g], NT)
        for k in range(DEP):
            for row in range(rows):
                base = (k * rows + row) * 8
                f_scr[row // 2, pl.ds(pl.multiple_of(k * OWN + at, 8), 8), (row % 2) * W : (row % 2 + 1) * W] = res[
                    base : base + 8
                ]
        return carry

    lax.fori_loop(0, 8, scatter, 0)

    def plane(r, carry):
        at = r * 4
        a = f_scr[pl.ds(at, 4)].reshape(4 * N, 2 * W).astype(BF)
        ay = dot(a, yf_ref[...]).astype(BF).reshape(4, N, 2 * W)
        stacked = jnp.concatenate(
            [jnp.concatenate([ay[b, :, p * W : (p + 1) * W] for p in range(2)], axis=0) for b in range(4)], axis=1
        )
        ax = dot(xf_ref[...], stacked)
        pot = pot_scr[r]
        pot = jnp.concatenate([jnp.concatenate([pot, pot], axis=0)] * 4, axis=1)
        bx = dot(xi_ref[...], (ax * pot).astype(BF)).astype(BF)
        lined = jnp.concatenate(
            [
                jnp.concatenate([bx[p * N : (p + 1) * N, b * W : (b + 1) * W] for p in range(2)], axis=1)
                for b in range(4)
            ],
            axis=0,
        )
        by = dot(lined, yi_ref[...])
        f_scr[pl.ds(at, 4)] = by.reshape(4, N, 2 * W)
        return carry

    lax.fori_loop(0, DEP, plane, 0)

    def gather(g, carry):
        at = pl.multiple_of(g * 8, 8)
        xl = rt_scr[0, pl.ds(at, 8), :]
        blocks = []
        for k in range(DEP):
            for row in range(rows):
                blocks.append(
                    f_scr[row // 2, pl.ds(pl.multiple_of(k * OWN + at, 8), 8), (row % 2) * W : (row % 2 + 1) * W]
                )
        lhs = jnp.concatenate(blocks, axis=0).astype(BF)
        res = dot(lhs, oh_scr[g])
        keep = [xl == k for k in range(DEP)]
        for row in range(rows):
            total = jnp.zeros((8, STK), F32)
            for k in range(DEP):
                base = (k * rows + row) * 8
                one = jnp.zeros((8, STK), F32)
                for d in range(8):
                    one = jnp.where(sub == d, res[base : base + 8, STK * d : STK * (d + 1)], one)
                total = jnp.where(keep[k], one, total)
            rt_scr[EXT + row, pl.ds(at, 8), :] = total
        return carry

    lax.fori_loop(0, 8, gather, 0)
    e = ext_ref[...]
    hi = e.astype(BF).astype(F32)
    mid = (e - hi).astype(BF).astype(F32)
    lo = e - hi - mid
    rt_scr[0] = hi
    rt_scr[1] = mid
    rt_scr[2] = lo
    out_ref[...] = jnp.swapaxes(rt_scr[...], 0, 1).astype(BF)


def wave_kernel(in_ref, orb_ref, slot_ref, col_ref, zi_ref, out_ref, sum_ref):
    npw = slot_ref.shape[1]
    rt = jnp.swapaxes(in_ref[...].astype(F32), 0, 1)
    sum_ref[...] = jnp.sum(rt[0] + rt[1] + rt[2], axis=0, keepdims=True)
    cols = []
    for b in range(4):
        cols.append(
            jnp.concatenate([rt[EXT + r * 8 + 2 * b + p] for p in range(2) for r in range(DEP)], axis=0)
        )
    spectrum = jnp.concatenate(cols, axis=1).astype(BF)
    sticks = dot(spectrum, zi_ref[...], TN).astype(BF)
    x, y = column_coords(col_ref[...])
    x = jnp.where(x >= N // 2, x - N, x)
    y = jnp.where(y >= N // 2, y - N, y)
    square = x * x + y * y
    square = jnp.sum(jnp.where(iota((STK, STK), 0) == iota((STK, STK), 1), square, 0.0), axis=1, keepdims=True)
    half = 512

    def pick(i, carry):
        at = pl.multiple_of(i * half, half)
        slot = slot_ref[:, pl.ds(at, half)]
        z = slot >> 7
        hot = jnp.where(iota((W, half), 0) == z, 1.0, 0.0).astype(BF)
        hit = iota((STK, half), 0) == (slot & (STK - 1))
        fz = jnp.where(z >= N // 2, z - N, z).astype(F32)
        kinetic = (fz * fz + jnp.sum(jnp.where(hit, square, 0.0), axis=0, keepdims=True)) * (2.0 / (N * N))
        lines = []
        for p in range(2):
            res = dot(sticks[:, p * W : (p + 1) * W], hot)
            for b in range(4):
                lines.append(
                    jnp.sum(jnp.where(hit, res[b * STK : (b + 1) * STK], 0.0), axis=0, keepdims=True)
                )
        for b in range(4):
            for p in range(2):
                j = 2 * b + p
                coeff = orb_ref[j : j + 1, pl.ds(at, half)].astype(F32)
                lines[p * 4 + b] = lines[p * 4 + b] + kinetic * coeff
        done = jnp.concatenate([lines[p * 4 + b] for b in range(4) for p in range(2)], axis=0)
        out_ref[:, pl.ds(at, half)] = done.astype(BF)
        return carry

    lax.fori_loop(0, npw // half, pick, 0)


def overlap_kernel(sub_ref, prev_ref, out_ref):
    out_ref[...] = dot(sub_ref[...], prev_ref[...], NT)


def call(kernel, outs, scratch, *args):
    return pl.pallas_call(
        kernel,
        out_shape=outs,
        scratch_shapes=scratch,
        compiler_params=pltpu.CompilerParams(vmem_limit_bytes=56 << 20),
    )(*args)


def stage_pack(orb, slot, col):
    npw = slot.shape[1]
    return call(
        pack_kernel,
        jax.ShapeDtypeStruct((OWN, EXT + 8 * DEP, STK), BF),
        [pltpu.VMEM((2 * W, npw), BF), pltpu.VMEM((512, npw), BF)],
        orb, slot, col, jnp.asarray(tables()["zf"]),
    )


def stage_plane(got, ext, pot):
    t = tables()
    return call(
        plane_kernel,
        jax.ShapeDtypeStruct((OWN, EXT + 8 * DEP, STK), BF),
        [
            pltpu.VMEM((EXT + 8 * DEP, OWN, STK), F32),
            pltpu.VMEM((8, W, 8 * STK), BF),
            pltpu.VMEM((8 * 8 * DEP * DEP, 8 * STK), BF),
            pltpu.VMEM((4 * DEP, N, 2 * W), F32),
            pltpu.VMEM((DEP, N, W), F32),
        ],
        got, ext, pot, *[jnp.asarray(t[k]) for k in ("yf", "xf", "xi", "yi")],
    )


def stage_wave(got, orb, slot, col):
    return call(
        wave_kernel,
        (jax.ShapeDtypeStruct(orb.shape, BF), jax.ShapeDtypeStruct((1, STK), F32)),
        [],
        got, orb, slot, col, jnp.asarray(tables()["zi"]),
    )


def per_device(orbitals, sphere_slot, stick_column, potential, subspace, previous):
    npw = sphere_slot.shape[0]
    orb = orbitals.reshape(8, npw)
    slot = sphere_slot.reshape(1, npw)
    col = stick_column.reshape(1, STK)
    send = stage_pack(orb, slot, col)
    got = lax.all_to_all(send, "fft", 0, 0, tiled=True)
    copies = jnp.broadcast_to(previous.reshape(1, 8, npw), (4, 8, npw))
    prev = lax.all_to_all(copies, "band", 0, 0, tiled=True).reshape(32, npw)
    raw = call(overlap_kernel, jax.ShapeDtypeStruct((32, 32), F32), [], subspace.reshape(32, npw), prev)
    raw = raw.reshape(16, 2, 16, 2)
    over = jnp.stack([raw[:, 0, :, 0] + raw[:, 1, :, 1], raw[:, 0, :, 1] - raw[:, 1, :, 0]])
    over = over.reshape(2, 16, 4, 4).transpose(2, 1, 0, 3).reshape(4, 16, 8)
    over = lax.all_to_all(over, "band", 0, 0, tiled=True).reshape(OWN, 8)
    ext = jnp.pad(over, ((0, 0), (0, STK - 8)))
    back = stage_plane(got, ext, potential)
    back = lax.all_to_all(back, "fft", 0, 0, tiled=True)
    applied, total = stage_wave(back, orb, slot, col)
    return applied.reshape(orbitals.shape), total[:, :8].reshape(2, 1, 4)


def solution(mesh):
    return jax.shard_map(
        per_device,
        mesh=mesh,
        in_specs=(
            P("band", None, "fft"),
            P("fft"),
            P("fft"),
            P("fft", None, None),
            P("band", None, "fft"),
            P("band", None, "fft"),
        ),
        out_specs=(P("band", None, "fft"), P(None, "fft", "band")),
        check_vma=False,
    )
```

```python
import functools
import math

import jax
import jax.numpy as jnp
import numpy as np
from jax import lax
from jax.experimental import pallas as pl
from jax.experimental.pallas import tpu as pltpu
from jax.sharding import PartitionSpec as P


BF = jnp.bfloat16
F32 = jnp.float32
N = 192
OWN = 64
DEP = N // OWN
STK = 128
W = 256
EXT = 8
NT = (((1,), (1,)), ((), ()))
TN = (((0,), (0,)), ((), ()))


def dot(a, b, dims=(((1,), (0,)), ((), ()))):
    return lax.dot_general(a, b, dims, preferred_element_type=F32)


@functools.cache
def tables():
    def trig(rows, cols, scale):
        angle = (np.outer(rows, cols) % N) * (2.0 * math.pi / N)
        return np.cos(angle) * scale, np.sin(angle) * scale

    nat = np.arange(N)
    dealt = (np.arange(DEP)[:, None] + DEP * np.arange(OWN)[None, :]).reshape(-1)

    def wide(a, rows, cols):
        out = np.zeros((rows, cols))
        out[: a.shape[0], : a.shape[1]] = a
        return out

    def left(rows, cols, scale, sign, width):
        c, s = trig(rows, cols, scale)
        c, s = wide(c, N, width), wide(s * sign, N, width)
        return np.block([[c, -s], [s, c]])

    def right(rows, cols, scale, sign, height, width):
        c, s = trig(rows, cols, scale)
        c, s = wide(c, height, width), wide(s * sign, height, width)
        return np.block([[c, s], [-s, c]])

    inv = 1.0 / N
    out = {
        "zf": left(dealt, nat, 1.0, 1.0, W),
        "yf": right(nat, nat, 1.0, 1.0, W, W),
        "xf": left(nat, dealt, 1.0, 1.0, N),
        "xi": left(dealt, nat, inv, -1.0, N),
        "yi": right(nat, nat, inv, -1.0, W, W),
        "zi": right(dealt, nat, inv, -1.0, N, W),
    }
    return {k: v.astype(np.float32).astype(BF) for k, v in out.items()}


def iota(shape, dim):
    return lax.broadcasted_iota(jnp.int32, shape, dim)


def column_coords(col):
    c = col.astype(F32)
    x = jnp.floor((c + 0.5) * (1.0 / N))
    return x, c - x * N


def pack_kernel(orb_ref, slot_ref, col_ref, zf_ref, out_ref, a_scr, b_scr):
    npw = slot_ref.shape[1]
    slot = slot_ref[...]
    low = slot & 63
    high = ((slot >> 6) & 1) * W + (slot >> 7)
    half = 1024
    for i in range(0, npw, half):
        cut = slice(i, i + half)
        a_scr[:, cut] = jnp.where(iota((2 * W, half), 0) == high[:, cut], 1.0, 0.0).astype(BF)
        hit = iota((64, half), 0) == low[:, cut]
        for j in range(8):
            row = orb_ref[j // 2, j % 2 : j % 2 + 1, cut].astype(F32)
            b_scr[64 * j : 64 * (j + 1), cut] = jnp.where(hit, row, 0.0).astype(BF)
    grid = dot(b_scr[...], a_scr[...], NT).astype(BF)
    rows = []
    for b in range(4):
        for h in range(2):
            rows.append(
                jnp.concatenate(
                    [grid[64 * (2 * b + p) : 64 * (2 * b + p + 1), W * h : W * (h + 1)] for p in range(2)],
                    axis=1,
                )
            )
    stick = jnp.concatenate(rows, axis=0)
    wave = dot(zf_ref[...], stick, NT)
    x, y = column_coords(col_ref[...])
    xl = x - DEP * jnp.floor((x + 0.5) * (1.0 / DEP))
    ext = jnp.where(iota((EXT, STK), 0) == 0, xl, jnp.where(iota((EXT, STK), 0) == 1, y, 0.0))
    parts = [jnp.broadcast_to(ext[e : e + 1, :], (OWN, STK)) for e in range(EXT)]
    for r in range(DEP):
        for b in range(4):
            for p in range(2):
                base = p * N + r * OWN
                parts.append(wave[base : base + OWN, STK * b : STK * (b + 1)])
    out_ref[...] = jnp.swapaxes(jnp.stack(parts, axis=0), 0, 1).astype(BF)


def plane_kernel(
    in_ref, ext_ref, pot_ref, yf_ref, xf_ref, xi_ref, yi_ref, out_ref, rt_scr, oh_scr, lhs_scr, f_scr, pot_scr
):
    rows = 8 * DEP
    rt_scr[...] = jnp.swapaxes(in_ref[...].astype(F32), 0, 1)
    pot_scr[...] = jnp.zeros(pot_scr.shape, F32)
    pot_scr[:, :, :N] = pot_ref[...]
    sub = iota((8, STK), 0)

    def scatter(g, carry):
        at = pl.multiple_of(g * 8, 8)
        xl = rt_scr[0, pl.ds(at, 8), :]
        y = rt_scr[1, pl.ds(at, 8), :].astype(jnp.int32)
        for d in range(8):
            oh_scr[g, :, STK * d : STK * (d + 1)] = jnp.where(iota((W, STK), 0) == y[d : d + 1, :], 1.0, 0.0).astype(BF)
        for k in range(DEP):
            for row in range(0, rows, 2):
                v = [jnp.where(xl == k, rt_scr[EXT + row + t, pl.ds(at, 8), :], 0.0) for t in range(2)]
                for d in range(8):
                    block = jnp.concatenate([jnp.where(sub == d, u, 0.0) for u in v], axis=0).astype(BF)
                    base = (k * rows + row) * 8
                    lhs_scr[base : base + 16, STK * d : STK * (d + 1)] = block
        res = dot(lhs_scr[...], oh_scr[g], NT)
        for k in range(DEP):
            for row in range(rows):
                base = (k * rows + row) * 8
                f_scr[row // 2, pl.ds(pl.multiple_of(k * OWN + at, 8), 8), (row % 2) * W : (row % 2 + 1) * W] = res[
                    base : base + 8
                ]
        return carry

    lax.fori_loop(0, 8, scatter, 0)

    def plane(r, carry):
        at = r * 4
        a = f_scr[pl.ds(at, 4)].reshape(4 * N, 2 * W).astype(BF)
        ay = dot(a, yf_ref[...]).astype(BF).reshape(4, N, 2 * W)
        stacked = jnp.concatenate(
            [jnp.concatenate([ay[b, :, p * W : (p + 1) * W] for p in range(2)], axis=0) for b in range(4)], axis=1
        )
        ax = dot(xf_ref[...], stacked)
        pot = pot_scr[r]
        pot = jnp.concatenate([jnp.concatenate([pot, pot], axis=0)] * 4, axis=1)
        bx = dot(xi_ref[...], (ax * pot).astype(BF)).astype(BF)
        lined = jnp.concatenate(
            [
                jnp.concatenate([bx[p * N : (p + 1) * N, b * W : (b + 1) * W] for p in range(2)], axis=1)
                for b in range(4)
            ],
            axis=0,
        )
        by = dot(lined, yi_ref[...])
        f_scr[pl.ds(at, 4)] = by.reshape(4, N, 2 * W)
        return carry

    lax.fori_loop(0, DEP, plane, 0)

    def gather(g, carry):
        at = pl.multiple_of(g * 8, 8)
        xl = rt_scr[0, pl.ds(at, 8), :]
        blocks = []
        for k in range(DEP):
            for row in range(rows):
                blocks.append(
                    f_scr[row // 2, pl.ds(pl.multiple_of(k * OWN + at, 8), 8), (row % 2) * W : (row % 2 + 1) * W]
                )
        lhs = jnp.concatenate(blocks, axis=0).astype(BF)
        res = dot(lhs, oh_scr[g])
        keep = [xl == k for k in range(DEP)]
        for row in range(rows):
            total = jnp.zeros((8, STK), F32)
            for k in range(DEP):
                base = (k * rows + row) * 8
                one = jnp.zeros((8, STK), F32)
                for d in range(8):
                    one = jnp.where(sub == d, res[base : base + 8, STK * d : STK * (d + 1)], one)
                total = jnp.where(keep[k], one, total)
            rt_scr[EXT + row, pl.ds(at, 8), :] = total
        return carry

    lax.fori_loop(0, 8, gather, 0)
    e = ext_ref[...]
    hi = e.astype(BF).astype(F32)
    mid = (e - hi).astype(BF).astype(F32)
    lo = e - hi - mid
    rt_scr[0] = hi
    rt_scr[1] = mid
    rt_scr[2] = lo
    out_ref[...] = jnp.swapaxes(rt_scr[...], 0, 1).astype(BF)


def fold_kernel(in_ref, out_ref):
    e = jnp.swapaxes(in_ref[:, :EXT, :].astype(F32), 0, 1)
    out_ref[...] = jnp.sum(e[0] + e[1] + e[2], axis=0, keepdims=True)


def wave_kernel(in_ref, orb_ref, slot_ref, col_ref, zi_ref, out_ref):
    npw = slot_ref.shape[1]
    rt = jnp.swapaxes(in_ref[...].astype(F32), 0, 1)
    cols = []
    for b in range(4):
        cols.append(
            jnp.concatenate([rt[EXT + r * 8 + 2 * b + p] for p in range(2) for r in range(DEP)], axis=0)
        )
    spectrum = jnp.concatenate(cols, axis=1).astype(BF)
    sticks = dot(spectrum, zi_ref[...], TN).astype(BF)
    x, y = column_coords(col_ref[...])
    x = jnp.where(x >= N // 2, x - N, x)
    y = jnp.where(y >= N // 2, y - N, y)
    square = x * x + y * y
    square = jnp.sum(jnp.where(iota((STK, STK), 0) == iota((STK, STK), 1), square, 0.0), axis=1, keepdims=True)
    half = 512

    def pick(i, carry):
        at = pl.multiple_of(i * half, half)
        slot = slot_ref[:, pl.ds(at, half)]
        z = slot >> 7
        hot = jnp.where(iota((W, half), 0) == z, 1.0, 0.0).astype(BF)
        hit = iota((STK, half), 0) == (slot & (STK - 1))
        fz = jnp.where(z >= N // 2, z - N, z).astype(F32)
        kinetic = (fz * fz + jnp.sum(jnp.where(hit, square, 0.0), axis=0, keepdims=True)) * (2.0 / (N * N))
        lines = []
        for p in range(2):
            res = dot(sticks[:, p * W : (p + 1) * W], hot)
            for b in range(4):
                lines.append(
                    jnp.sum(jnp.where(hit, res[b * STK : (b + 1) * STK], 0.0), axis=0, keepdims=True)
                )
        for b in range(4):
            for p in range(2):
                coeff = orb_ref[b, p : p + 1, pl.ds(at, half)].astype(F32)
                lines[p * 4 + b] = lines[p * 4 + b] + kinetic * coeff
        for b in range(4):
            done = jnp.concatenate([lines[b], lines[4 + b]], axis=0)
            out_ref[b, :, pl.ds(at, half)] = done.astype(BF)
        return carry

    lax.fori_loop(0, npw // half, pick, 0)


def overlap_kernel(sub_ref, *refs):
    out_ref = refs[-1]
    sub = sub_ref[...].astype(F32)
    sub = jnp.concatenate([sub[:, 0], sub[:, 1]], axis=1).astype(BF)
    rows = []
    for ref in refs[:-1]:
        prev = ref[...].astype(F32)
        re, im = prev[:, 0], prev[:, 1]
        rows.append(jnp.concatenate([re, im], axis=1))
        rows.append(jnp.concatenate([im, -re], axis=1))
    res = dot(sub, jnp.concatenate(rows, axis=0).astype(BF), NT)
    out_ref[...] = jnp.zeros(out_ref.shape, F32)
    for s in range(4):
        out_ref[16 * s : 16 * (s + 1), :8] = res[:, 8 * s : 8 * (s + 1)]


def call(kernel, outs, scratch, *args):
    return pl.pallas_call(
        kernel,
        out_shape=outs,
        scratch_shapes=scratch,
        compiler_params=pltpu.CompilerParams(vmem_limit_bytes=56 << 20),
    )(*args)


def stage_pack(orb, slot, col):
    npw = slot.shape[1]
    return call(
        pack_kernel,
        jax.ShapeDtypeStruct((OWN, EXT + 8 * DEP, STK), BF),
        [pltpu.VMEM((2 * W, npw), BF), pltpu.VMEM((512, npw), BF)],
        orb, slot, col, jnp.asarray(tables()["zf"]),
    )


def stage_plane(got, ext, pot):
    t = tables()
    return call(
        plane_kernel,
        jax.ShapeDtypeStruct((OWN, EXT + 8 * DEP, STK), BF),
        [
            pltpu.VMEM((EXT + 8 * DEP, OWN, STK), F32),
            pltpu.VMEM((8, W, 8 * STK), BF),
            pltpu.VMEM((8 * 8 * DEP * DEP, 8 * STK), BF),
            pltpu.VMEM((4 * DEP, N, 2 * W), F32),
            pltpu.VMEM((DEP, N, W), F32),
        ],
        got, ext, pot, *[jnp.asarray(t[k]) for k in ("yf", "xf", "xi", "yi")],
    )


def stage_wave(got, orb, slot, col):
    return call(
        wave_kernel,
        jax.ShapeDtypeStruct(orb.shape, BF),
        [],
        got, orb, slot, col, jnp.asarray(tables()["zi"]),
    )


def per_device(orbitals, sphere_slot, stick_column, potential, subspace, previous):
    npw = sphere_slot.shape[0]
    slot = sphere_slot.reshape(1, npw)
    col = stick_column.reshape(1, STK)
    send = stage_pack(orbitals, slot, col)
    got = lax.all_to_all(send, "fft", 0, 0, tiled=True)
    others = [lax.ppermute(previous, "band", [(g, (g + k) % 4) for g in range(4)]) for k in (1, 2, 3)]
    shape = jax.ShapeDtypeStruct((OWN, STK), F32)
    ext = call(overlap_kernel, shape, [], subspace, previous, *others)
    back = stage_plane(got, ext, potential)
    back = lax.all_to_all(back, "fft", 0, 0, tiled=True)
    total = call(fold_kernel, jax.ShapeDtypeStruct((1, STK), F32), [], back)
    moves = [
        (OWN * g + 16 * k + r, OWN * ((g - k) % 4) + 16 * g + r)
        for g in range(4)
        for k in range(4)
        for r in range(16)
    ]
    total = lax.ppermute(total, ("band", "fft"), moves)
    applied = stage_wave(back, orbitals, slot, col)
    return applied, total[:, :8].reshape(2, 1, 4)


def solution(mesh):
    return jax.shard_map(
        per_device,
        mesh=mesh,
        in_specs=(
            P("band", None, "fft"),
            P("fft"),
            P("fft"),
            P("fft", None, None),
            P("band", None, "fft"),
            P("band", None, "fft"),
        ),
        out_specs=(P("band", None, "fft"), P(None, "fft", "band")),
        check_vma=False,
    )
```

```python
import functools
import math

import jax
import jax.numpy as jnp
import numpy as np
from jax import lax
from jax.experimental import pallas as pl
from jax.experimental.pallas import tpu as pltpu
from jax.sharding import PartitionSpec as P


BF = jnp.bfloat16
F32 = jnp.float32
N = 192
OWN = 64
DEP = N // OWN
STK = 128
W = 256
EXT = 8
MSG = EXT + 8 * DEP
NT = (((1,), (1,)), ((), ()))
TN = (((0,), (0,)), ((), ()))


def dot(a, b, dims=(((1,), (0,)), ((), ()))):
    return lax.dot_general(a, b, dims, preferred_element_type=F32)


@functools.cache
def tables():
    def trig(rows, cols, scale):
        angle = (np.outer(rows, cols) % N) * (2.0 * math.pi / N)
        return np.cos(angle) * scale, np.sin(angle) * scale

    nat = np.arange(N)
    dealt = (np.arange(DEP)[:, None] + DEP * np.arange(OWN)[None, :]).reshape(-1)

    def wide(a, rows, cols):
        out = np.zeros((rows, cols))
        out[: a.shape[0], : a.shape[1]] = a
        return out

    def left(rows, cols, scale, sign, width):
        c, s = trig(rows, cols, scale)
        c, s = wide(c, N, width), wide(s * sign, N, width)
        return np.block([[c, -s], [s, c]])

    def right(rows, cols, scale, sign, height, width):
        c, s = trig(rows, cols, scale)
        c, s = wide(c, height, width), wide(s * sign, height, width)
        return np.block([[c, s], [-s, c]])

    inv = 1.0 / N
    out = {
        "zf": left(dealt, nat, 1.0, 1.0, W),
        "yf": right(nat, nat, 1.0, 1.0, W, W),
        "xf": left(nat, dealt, 1.0, 1.0, N),
        "xi": left(dealt, nat, inv, -1.0, N),
        "yi": right(nat, nat, inv, -1.0, W, W),
        "zi": right(dealt, nat, inv, -1.0, N, W),
    }
    return {k: v.astype(np.float32).astype(BF) for k, v in out.items()}


def iota(shape, dim):
    return lax.broadcasted_iota(jnp.int32, shape, dim)


def column_coords(col):
    c = col.astype(F32)
    x = jnp.floor((c + 0.5) * (1.0 / N))
    return x, c - x * N


def pack_kernel(orb_ref, slot_ref, col_ref, zf_ref, out_ref, a_scr, b_scr, m_scr):
    npw = slot_ref.shape[1]
    slot = slot_ref[...]
    low = slot & 63
    high = ((slot >> 6) & 1) * W + (slot >> 7)
    half = 1024
    for i in range(0, npw, half):
        cut = slice(i, i + half)
        a_scr[:, cut] = jnp.where(iota((2 * W, half), 0) == high[:, cut], 1.0, 0.0).astype(BF)
        hit = iota((64, half), 0) == low[:, cut]
        for j in range(8):
            row = orb_ref[j // 2, j % 2 : j % 2 + 1, cut].astype(F32)
            b_scr[64 * j : 64 * (j + 1), cut] = jnp.where(hit, row, 0.0).astype(BF)
    grid = dot(b_scr[...], a_scr[...], NT).astype(BF)
    rows = []
    for b in range(4):
        for h in range(2):
            rows.append(
                jnp.concatenate(
                    [grid[64 * (2 * b + p) : 64 * (2 * b + p + 1), W * h : W * (h + 1)] for p in range(2)],
                    axis=1,
                )
            )
    stick = jnp.concatenate(rows, axis=0)
    wave = dot(zf_ref[...], stick, NT)
    x, y = column_coords(col_ref[...])
    xl = x - DEP * jnp.floor((x + 0.5) * (1.0 / DEP))
    ext = jnp.where(iota((EXT, STK), 0) == 0, xl, jnp.where(iota((EXT, STK), 0) == 1, y, 0.0))
    for r in range(DEP):
        for j in range(8):
            base = (j % 2) * N + r * OWN
            m_scr[r, pl.ds(j, OWN, stride=8), :] = wave[base : base + OWN, STK * (j // 2) : STK * (j // 2 + 1)]
    parts = [jnp.broadcast_to(ext[None], (OWN, EXT, STK))] + [m_scr[r].reshape(OWN, 8, STK) for r in range(DEP)]
    out_ref[...] = jnp.concatenate(parts, axis=1).astype(BF)


def plane_kernel(
    in_ref, ext_ref, pot_hbm, yf_hbm, xf_hbm, xi_hbm, yi_hbm, out_ref, oh_scr, lo_scr, hi_scr, pot_scr, yf, xf, xi, yi, sems
):
    rows = 8 * DEP
    copies = [
        pltpu.make_async_copy(src, dst, sems.at[i])
        for i, (src, dst) in enumerate(
            [(yf_hbm, yf), (xf_hbm, xf), (pot_hbm, pot_scr), (xi_hbm, xi), (yi_hbm, yi)]
        )
    ]
    for copy in copies:
        copy.start()
    halves = (lo_scr, hi_scr)

    def scatter(i, carry):
        for u in range(16):
            d = i * 16 + u
            m = in_ref[d].astype(F32)
            xl, y = m[0:1], m[1:2].astype(jnp.int32)
            hot = jnp.where(iota((N, STK), 0) == y, 1.0, 0.0).astype(BF)
            hot = jnp.concatenate([hot, jnp.zeros((W - N, STK), BF)], axis=0)
            oh_scr[d] = hot
            lhs = jnp.concatenate([jnp.where(xl == k, m[EXT:], 0.0) for k in range(DEP)], axis=0).astype(BF)
            res = dot(lhs, hot, NT)
            for k in range(DEP):
                for r in range(DEP):
                    base = k * rows + r * 8
                    for h in range(2):
                        at = pl.multiple_of((r * N + k * OWN + d) * 8, 8)
                        halves[h][pl.ds(at, 8), :] = res[
                            base : base + 8, h * STK : (h + 1) * STK
                        ]
        return carry

    lax.fori_loop(0, OWN // 16, scatter, 0)
    for copy in copies:
        copy.wait()

    def plane(r, carry):
        at = r * 8 * N
        lined = []
        for b in range(4):
            parts = [
                half[pl.ds(at + 2 * b + p, N, stride=8), :].astype(BF) for p in range(2) for half in halves
            ]
            lined.append(jnp.concatenate(parts, axis=1))
        ay = dot(jnp.concatenate(lined, axis=0), yf[...]).astype(BF).reshape(4, N, 2 * W)
        stacked = jnp.concatenate(
            [jnp.concatenate([ay[b, :, p * W : (p + 1) * W] for p in range(2)], axis=0) for b in range(4)], axis=1
        )
        ax = dot(xf[...], stacked)
        pot = jnp.concatenate([pot_scr[r], jnp.zeros((N, W - N), F32)], axis=1)
        pot = jnp.concatenate([jnp.concatenate([pot, pot], axis=0)] * 4, axis=1)
        bx = dot(xi[...], (ax * pot).astype(BF)).astype(BF)
        lined = jnp.concatenate(
            [
                jnp.concatenate([bx[p * N : (p + 1) * N, b * W : (b + 1) * W] for p in range(2)], axis=1)
                for b in range(4)
            ],
            axis=0,
        )
        by = dot(lined, yi[...])
        for b in range(4):
            for p in range(2):
                for h in range(2):
                    halves[h][pl.ds(at + 2 * b + p, N, stride=8), :] = by[
                        b * N : (b + 1) * N, (2 * p + h) * STK : (2 * p + h + 1) * STK
                    ]
        return carry

    lax.fori_loop(0, DEP, plane, 0)
    spot = iota((EXT, STK), 0)

    def gather(i, carry):
        for u in range(8):
            pair = [i * 16 + 2 * u, i * 16 + 2 * u + 1]
            blocks = []
            for d in pair:
                for k in range(DEP):
                    for r in range(DEP):
                        blocks.append(
                            jnp.concatenate(
                                [
                                    half[pl.ds(pl.multiple_of((r * N + k * OWN + d) * 8, 8), 8), :]
                                    for half in halves
                                ],
                                axis=1,
                            )
                        )
            lhs = jnp.concatenate(blocks, axis=0).astype(BF)
            res = dot(lhs, jnp.concatenate([oh_scr[d] for d in pair], axis=1))
            for t, d in enumerate(pair):
                xl = in_ref[d, 0:8].astype(F32)[0:1]
                took = [
                    res[(t * DEP + k) * rows : (t * DEP + k + 1) * rows, t * STK : (t + 1) * STK] for k in range(DEP)
                ]
                field = jnp.where(xl == 0.0, took[0], jnp.where(xl == 1.0, took[1], took[2]))
                e = ext_ref[pl.ds(d, 1), :]
                top = e.astype(BF).astype(F32)
                mid = (e - top).astype(BF).astype(F32)
                low = e - top - mid
                head = jnp.where(spot == 0, top, jnp.where(spot == 1, mid, jnp.where(spot == 2, low, 0.0)))
                out_ref[d] = jnp.concatenate([head, field], axis=0).astype(BF)
        return carry

    lax.fori_loop(0, OWN // 16, gather, 0)


def fold_kernel(in_ref, out_ref):
    e = jnp.swapaxes(in_ref[:, :EXT, :].astype(F32), 0, 1)
    out_ref[...] = jnp.sum(e[0] + e[1] + e[2], axis=0, keepdims=True)


def wave_kernel(in_ref, orb_ref, slot_ref, col_ref, zi_ref, out_ref, m_scr):
    npw = slot_ref.shape[1]
    for r in range(DEP):
        m_scr[r] = in_ref[:, EXT + 8 * r : EXT + 8 * (r + 1), :].astype(F32).reshape(OWN * 8, STK)
    cols = []
    for b in range(4):
        picks = [m_scr[r, pl.ds(2 * b + p, OWN, stride=8), :] for p in range(2) for r in range(DEP)]
        cols.append(jnp.concatenate(picks, axis=0))
    spectrum = jnp.concatenate(cols, axis=1).astype(BF)
    sticks = dot(spectrum, zi_ref[...], TN).astype(BF)
    sticks = [
        jnp.concatenate(
            [
                jnp.concatenate(
                    [sticks[b * STK + 64 * h : b * STK + 64 * (h + 1), p * W : (p + 1) * W] for h in range(2)], axis=1
                )
                for b in range(4)
            ],
            axis=0,
        )
        for p in range(2)
    ]
    x, y = column_coords(col_ref[...])
    x = jnp.where(x >= N // 2, x - N, x)
    y = jnp.where(y >= N // 2, y - N, y)
    square = x * x + y * y
    square = jnp.sum(jnp.where(iota((STK, STK), 0) == iota((STK, STK), 1), square, 0.0), axis=1, keepdims=True)
    half = 512

    def pick(i, carry):
        at = pl.multiple_of(i * half, half)
        slot = slot_ref[:, pl.ds(at, half)]
        z = slot >> 7
        stick = slot & (STK - 1)
        hot = jnp.concatenate(
            [jnp.where(iota((W, half), 0) == jnp.where(stick >> 6 == h, z, -1), 1.0, 0.0).astype(BF) for h in range(2)],
            axis=0,
        )
        hit = iota((STK, half), 0) == stick
        low = iota((64, half), 0) == (stick & 63)
        fz = jnp.where(z >= N // 2, z - N, z).astype(F32)
        kinetic = (fz * fz + jnp.sum(jnp.where(hit, square, 0.0), axis=0, keepdims=True)) * (2.0 / (N * N))
        lines = []
        for p in range(2):
            res = dot(sticks[p], hot)
            for b in range(4):
                lines.append(jnp.sum(jnp.where(low, res[b * 64 : (b + 1) * 64], 0.0), axis=0, keepdims=True))
        for b in range(4):
            for p in range(2):
                coeff = orb_ref[b, p : p + 1, pl.ds(at, half)].astype(F32)
                lines[p * 4 + b] = lines[p * 4 + b] + kinetic * coeff
        for b in range(4):
            done = jnp.concatenate([lines[b], lines[4 + b]], axis=0)
            out_ref[b, :, pl.ds(at, half)] = done.astype(BF)
        return carry

    lax.fori_loop(0, npw // half, pick, 0, unroll=2)


def overlap_kernel(sub_ref, *refs):
    out_ref = refs[-1]
    sub = sub_ref[...].astype(F32)
    sub = jnp.concatenate([sub[:, 0], sub[:, 1]], axis=1).astype(BF)
    rows = []
    for ref in refs[:-1]:
        prev = ref[...].astype(F32)
        re, im = prev[:, 0], prev[:, 1]
        rows.append(jnp.concatenate([re, im], axis=1))
        rows.append(jnp.concatenate([im, -re], axis=1))
    res = dot(sub, jnp.concatenate(rows, axis=0).astype(BF), NT)
    out_ref[...] = jnp.zeros(out_ref.shape, F32)
    for s in range(4):
        out_ref[16 * s : 16 * (s + 1), :8] = res[:, 8 * s : 8 * (s + 1)]


def call(kernel, outs, scratch, *args):
    return pl.pallas_call(
        kernel,
        out_shape=outs,
        scratch_shapes=scratch,
        compiler_params=pltpu.CompilerParams(vmem_limit_bytes=56 << 20),
    )(*args)


def stage_pack(orb, slot, col):
    npw = slot.shape[1]
    return call(
        pack_kernel,
        jax.ShapeDtypeStruct((OWN, MSG, STK), BF),
        [pltpu.VMEM((2 * W, npw), BF), pltpu.VMEM((512, npw), BF), pltpu.VMEM((DEP, OWN * 8, STK), F32)],
        orb, slot, col, jnp.asarray(tables()["zf"]),
    )


def stage_plane(got, ext, pot):
    t = tables()
    names = ("yf", "xf", "xi", "yi")
    return pl.pallas_call(
        plane_kernel,
        out_shape=jax.ShapeDtypeStruct((OWN, MSG, STK), BF),
        in_specs=[pl.BlockSpec(memory_space=pltpu.VMEM)] * 2 + [pl.BlockSpec(memory_space=pl.ANY)] * 5,
        scratch_shapes=[
            pltpu.VMEM((OWN, W, STK), BF),
            pltpu.VMEM((8 * DEP * N, STK), F32),
            pltpu.VMEM((8 * DEP * N, STK), F32),
            pltpu.VMEM((DEP, N, N), F32),
            *[pltpu.VMEM(t[k].shape, BF) for k in names],
            pltpu.SemaphoreType.DMA((5,)),
        ],
        compiler_params=pltpu.CompilerParams(vmem_limit_bytes=56 << 20),
    )(got, ext, pot, *[jnp.asarray(t[k]) for k in names])


def stage_wave(got, orb, slot, col):
    return call(
        wave_kernel,
        jax.ShapeDtypeStruct(orb.shape, BF),
        [pltpu.VMEM((DEP, OWN * 8, STK), F32)],
        got, orb, slot, col, jnp.asarray(tables()["zi"]),
    )


def per_device(orbitals, sphere_slot, stick_column, potential, subspace, previous):
    npw = sphere_slot.shape[0]
    slot = sphere_slot.reshape(1, npw)
    col = stick_column.reshape(1, STK)
    send = stage_pack(orbitals, slot, col)
    got = lax.all_to_all(send, "fft", 0, 0, tiled=True)
    others = [lax.ppermute(previous, "band", [(g, (g + k) % 4) for g in range(4)]) for k in (1, 2, 3)]
    shape = jax.ShapeDtypeStruct((OWN, STK), F32)
    ext = call(overlap_kernel, shape, [], subspace, previous, *others)
    back = stage_plane(got, ext, potential)
    back = lax.all_to_all(back, "fft", 0, 0, tiled=True)
    total = call(fold_kernel, jax.ShapeDtypeStruct((1, STK), F32), [], back)
    moves = [
        (OWN * g + 16 * k + r, OWN * ((g - k) % 4) + 16 * g + r)
        for g in range(4)
        for k in range(4)
        for r in range(16)
    ]
    total = lax.ppermute(total, ("band", "fft"), moves)
    applied = stage_wave(back, orbitals, slot, col)
    return applied, total[:, :8].reshape(2, 1, 4)


def solution(mesh):
    return jax.shard_map(
        per_device,
        mesh=mesh,
        in_specs=(
            P("band", None, "fft"),
            P("fft"),
            P("fft"),
            P("fft", None, None),
            P("band", None, "fft"),
            P("band", None, "fft"),
        ),
        out_specs=(P("band", None, "fft"), P(None, "fft", "band")),
        check_vma=False,
    )
```

```python
import functools
import math

import jax
import jax.numpy as jnp
import numpy as np
from jax import lax
from jax.experimental import pallas as pl
from jax.experimental.pallas import tpu as pltpu
from jax.sharding import PartitionSpec as P


BF = jnp.bfloat16
F32 = jnp.float32
N = 192
OWN = 64
DEP = N // OWN
STK = 128
W = 256
ROWS = 8 * DEP
EXT = 2
MSG = EXT + ROWS
GRP = 16
NT = (((1,), (1,)), ((), ()))
TN = (((0,), (0,)), ((), ()))


def dot(a, b, dims=(((1,), (0,)), ((), ()))):
    return lax.dot_general(a, b, dims, preferred_element_type=F32)


@functools.cache
def tables():
    def trig(rows, cols, scale):
        angle = (np.outer(rows, cols) % N) * (2.0 * math.pi / N)
        return np.cos(angle) * scale, np.sin(angle) * scale

    nat = np.arange(N)
    dealt = (np.arange(DEP)[:, None] + DEP * np.arange(OWN)[None, :]).reshape(-1)

    def wide(a, rows, cols):
        out = np.zeros((rows, cols))
        out[: a.shape[0], : a.shape[1]] = a
        return out

    def left(rows, cols, scale, sign, width):
        c, s = trig(rows, cols, scale)
        c, s = wide(c, N, width), wide(s * sign, N, width)
        return np.block([[c, -s], [s, c]])

    def right(rows, cols, scale, sign, height, width):
        c, s = trig(rows, cols, scale)
        c, s = wide(c, height, width), wide(s * sign, height, width)
        return np.block([[c, s], [-s, c]])

    inv = 1.0 / N
    out = {
        "zf": left(dealt, nat, 1.0, 1.0, W),
        "yf": right(nat, nat, 1.0, 1.0, W, W),
        "xf": left(nat, dealt, 1.0, 1.0, N),
        "xi": left(dealt, nat, inv, -1.0, N),
        "yi": right(nat, nat, inv, -1.0, W, W),
        "zi": right(dealt, nat, inv, -1.0, N, W),
    }
    return {k: v.astype(np.float32).astype(BF) for k, v in out.items()}


def iota(shape, dim):
    return lax.broadcasted_iota(jnp.int32, shape, dim)


def column_coords(col):
    c = col.astype(F32)
    x = jnp.floor((c + 0.5) * (1.0 / N))
    return x, c - x * N


def fetch(sems, *pairs):
    copies = [pltpu.make_async_copy(src, dst, sems.at[i]) for i, (src, dst) in enumerate(pairs)]
    for copy in copies:
        copy.start()
    return copies


def pack_kernel(
    orb_hbm, slot_hbm, col_hbm, zf_hbm, out_ref, a_scr, b_scr, m_scr, orb_ref, slot_ref, col_ref, zf_ref, sems
):
    copies = fetch(sems, (slot_hbm, slot_ref), (orb_hbm, orb_ref), (col_hbm, col_ref), (zf_hbm, zf_ref))
    npw = slot_ref.shape[1]
    copies[0].wait()
    slot = slot_ref[...]
    low = slot & 63
    high = ((slot >> 6) & 1) * W + (slot >> 7)
    half = 1024
    copies[1].wait()
    for i in range(0, npw, half):
        cut = slice(i, i + half)
        a_scr[:, cut] = jnp.where(iota((2 * W, half), 0) == high[:, cut], 1.0, 0.0).astype(BF)
        hit = iota((64, half), 0) == low[:, cut]
        for j in range(8):
            row = orb_ref[j // 2, j % 2 : j % 2 + 1, cut].astype(F32)
            b_scr[64 * j : 64 * (j + 1), cut] = jnp.where(hit, row, 0.0).astype(BF)
    grid = dot(b_scr[...], a_scr[...], NT).astype(BF)
    rows = []
    for b in range(4):
        for h in range(2):
            rows.append(
                jnp.concatenate(
                    [grid[64 * (2 * b + p) : 64 * (2 * b + p + 1), W * h : W * (h + 1)] for p in range(2)],
                    axis=1,
                )
            )
    stick = jnp.concatenate(rows, axis=0)
    copies[2].wait()
    copies[3].wait()
    wave = dot(zf_ref[...], stick, NT)
    x, y = column_coords(col_ref[...])
    xl = x - DEP * jnp.floor((x + 0.5) * (1.0 / DEP))
    ext = jnp.concatenate([xl, y], axis=0)
    for r in range(DEP):
        for j in range(8):
            base = (j % 2) * N + r * OWN
            m_scr[r, pl.ds(j, OWN, stride=8), :] = wave[base : base + OWN, STK * (j // 2) : STK * (j // 2 + 1)]

    def pour(i, carry):
        at = pl.multiple_of(i * GRP * 8, 8)
        block = [m_scr[r, pl.ds(at, GRP * 8), :] for r in range(DEP)]
        parts = []
        for u in range(GRP):
            parts += [ext] + [block[r][8 * u : 8 * u + 8] for r in range(DEP)]
        out_ref[pl.ds(pl.multiple_of(i * GRP * MSG, 16), GRP * MSG), :] = jnp.concatenate(parts, axis=0).astype(BF)
        return carry

    lax.fori_loop(0, OWN // GRP, pour, 0)


def plane_kernel(
    in_ref, pot_hbm, yf_hbm, xf_hbm, xi_hbm, yi_hbm, out_ref, oh_scr, xl_scr, lo_scr, hi_scr, pot_scr, yf, xf, xi, yi, sems
):
    rows = ROWS
    copies = fetch(sems, (yf_hbm, yf), (xf_hbm, xf), (pot_hbm, pot_scr), (xi_hbm, xi), (yi_hbm, yi))
    halves = (lo_scr, hi_scr)

    def scatter(i, carry):
        block = in_ref[pl.ds(pl.multiple_of(i * GRP * MSG, 16), GRP * MSG), :].astype(F32)
        for u in range(GRP):
            d = i * GRP + u
            m = block[MSG * u : MSG * (u + 1)]
            xl, y = m[0:1], m[1:2].astype(jnp.int32)
            xl_scr[pl.ds(d, 1), :] = xl
            hot = jnp.where(iota((N, STK), 0) == y, 1.0, 0.0).astype(BF)
            hot = jnp.concatenate([hot, jnp.zeros((W - N, STK), BF)], axis=0)
            oh_scr[d] = hot
            lhs = jnp.concatenate([jnp.where(xl == k, m[EXT:], 0.0) for k in range(DEP)], axis=0).astype(BF)
            res = dot(lhs, hot, NT)
            for k in range(DEP):
                for r in range(DEP):
                    base = k * rows + r * 8
                    for h in range(2):
                        at = pl.multiple_of((r * N + k * OWN + d) * 8, 8)
                        halves[h][pl.ds(at, 8), :] = res[
                            base : base + 8, h * STK : (h + 1) * STK
                        ]
        return carry

    lax.fori_loop(0, OWN // GRP, scatter, 0)
    for copy in copies:
        copy.wait()

    def plane(r, carry):
        at = r * 8 * N
        lined = []
        for b in range(4):
            parts = [
                half[pl.ds(at + 2 * b + p, N, stride=8), :].astype(BF) for p in range(2) for half in halves
            ]
            lined.append(jnp.concatenate(parts, axis=1))
        ay = dot(jnp.concatenate(lined, axis=0), yf[...]).astype(BF).reshape(4, N, 2 * W)
        stacked = jnp.concatenate(
            [jnp.concatenate([ay[b, :, p * W : (p + 1) * W] for p in range(2)], axis=0) for b in range(4)], axis=1
        )
        ax = dot(xf[...], stacked)
        pot = jnp.concatenate([pot_scr[r], jnp.zeros((N, W - N), F32)], axis=1)
        pot = jnp.concatenate([jnp.concatenate([pot, pot], axis=0)] * 4, axis=1)
        bx = dot(xi[...], (ax * pot).astype(BF)).astype(BF)
        lined = jnp.concatenate(
            [
                jnp.concatenate([bx[p * N : (p + 1) * N, b * W : (b + 1) * W] for p in range(2)], axis=1)
                for b in range(4)
            ],
            axis=0,
        )
        by = dot(lined, yi[...])
        for b in range(4):
            for p in range(2):
                for h in range(2):
                    halves[h][pl.ds(at + 2 * b + p, N, stride=8), :] = by[
                        b * N : (b + 1) * N, (2 * p + h) * STK : (2 * p + h + 1) * STK
                    ]
        return carry

    lax.fori_loop(0, DEP, plane, 0)

    def gather(i, carry):
        parts = []
        for u in range(GRP // 2):
            pair = [i * GRP + 2 * u, i * GRP + 2 * u + 1]
            blocks = []
            for d in pair:
                for k in range(DEP):
                    for r in range(DEP):
                        blocks.append(
                            jnp.concatenate(
                                [
                                    half[pl.ds(pl.multiple_of((r * N + k * OWN + d) * 8, 8), 8), :]
                                    for half in halves
                                ],
                                axis=1,
                            )
                        )
            lhs = jnp.concatenate(blocks, axis=0).astype(BF)
            res = dot(lhs, jnp.concatenate([oh_scr[d] for d in pair], axis=1))
            for t, d in enumerate(pair):
                xl = xl_scr[pl.ds(d, 1), :]
                took = [
                    res[(t * DEP + k) * rows : (t * DEP + k + 1) * rows, t * STK : (t + 1) * STK] for k in range(DEP)
                ]
                field = jnp.where(xl == 0.0, took[0], jnp.where(xl == 1.0, took[1], took[2]))
                parts += [jnp.zeros((EXT, STK), F32), field]
        out_ref[pl.ds(pl.multiple_of(i * GRP * MSG, 16), GRP * MSG), :] = jnp.concatenate(parts, axis=0).astype(BF)
        return carry

    lax.fori_loop(0, OWN // GRP, gather, 0)


def wave_kernel(
    in_ref, orb_hbm, slot_hbm, col_hbm, zi_hbm, out_ref, sum_ref, m_scr, orb_ref, slot_ref, col_ref, zi_ref, sems
):
    copies = fetch(sems, (zi_hbm, zi_ref), (col_hbm, col_ref), (slot_hbm, slot_ref), (orb_hbm, orb_ref))
    npw = slot_ref.shape[1]

    def unpour(i, total):
        block = in_ref[pl.ds(pl.multiple_of(i * GRP * MSG, 16), GRP * MSG), :].astype(F32)
        for u in range(GRP):
            total = total + block[MSG * u : MSG * u + 1]
            for r in range(DEP):
                row = MSG * u + EXT + 8 * r
                m_scr[r, pl.ds(pl.multiple_of((i * GRP + u) * 8, 8), 8), :] = block[row : row + 8]
        return total

    total = lax.fori_loop(0, OWN // GRP, unpour, jnp.zeros((1, STK), F32))
    total = total[:, 0:8] + total[:, 8:16] + total[:, 16:24]
    sum_ref[...] = jnp.concatenate([total[:, 0:4], total[:, 4:8]], axis=0)
    cols = []
    for b in range(4):
        picks = [m_scr[r, pl.ds(2 * b + p, OWN, stride=8), :] for p in range(2) for r in range(DEP)]
        cols.append(jnp.concatenate(picks, axis=0))
    for copy in copies:
        copy.wait()
    spectrum = jnp.concatenate(cols, axis=1).astype(BF)
    sticks = dot(spectrum, zi_ref[...], TN).astype(BF)
    sticks = [
        jnp.concatenate(
            [
                jnp.concatenate(
                    [sticks[b * STK + 64 * h : b * STK + 64 * (h + 1), p * W : (p + 1) * W] for h in range(2)], axis=1
                )
                for b in range(4)
            ],
            axis=0,
        )
        for p in range(2)
    ]
    x, y = column_coords(col_ref[...])
    x = jnp.where(x >= N // 2, x - N, x)
    y = jnp.where(y >= N // 2, y - N, y)
    square = x * x + y * y
    square = jnp.sum(jnp.where(iota((STK, STK), 0) == iota((STK, STK), 1), square, 0.0), axis=1, keepdims=True)
    half = 512

    def pick(i, carry):
        at = pl.multiple_of(i * half, half)
        slot = slot_ref[:, pl.ds(at, half)]
        z = slot >> 7
        stick = slot & (STK - 1)
        hot = jnp.concatenate(
            [jnp.where(iota((W, half), 0) == jnp.where(stick >> 6 == h, z, -1), 1.0, 0.0).astype(BF) for h in range(2)],
            axis=0,
        )
        hit = iota((STK, half), 0) == stick
        low = iota((64, half), 0) == (stick & 63)
        fz = jnp.where(z >= N // 2, z - N, z).astype(F32)
        kinetic = (fz * fz + jnp.sum(jnp.where(hit, square, 0.0), axis=0, keepdims=True)) * (2.0 / (N * N))
        lines = []
        for p in range(2):
            res = dot(sticks[p], hot)
            for b in range(4):
                lines.append(jnp.sum(jnp.where(low, res[b * 64 : (b + 1) * 64], 0.0), axis=0, keepdims=True))
        for b in range(4):
            for p in range(2):
                coeff = orb_ref[b, p : p + 1, pl.ds(at, half)].astype(F32)
                lines[p * 4 + b] = lines[p * 4 + b] + kinetic * coeff
        for b in range(4):
            done = jnp.concatenate([lines[b], lines[4 + b]], axis=0)
            out_ref[b, :, pl.ds(at, half)] = done.astype(BF)
        return carry

    lax.fori_loop(0, npw // half, pick, 0, unroll=2)


def overlap_kernel(sub_ref, *refs):
    refs, out_refs = refs[:4], refs[4:]
    sub = sub_ref[...].astype(F32)
    sub = jnp.concatenate([sub[:, 0], sub[:, 1]], axis=1).astype(BF)
    rows = []
    for ref in refs:
        prev = ref[...].astype(F32)
        re, im = prev[:, 0], prev[:, 1]
        rows.append(jnp.concatenate([re, im], axis=1))
        rows.append(jnp.concatenate([im, -re], axis=1))
    res = dot(sub, jnp.concatenate(rows, axis=0).astype(BF), NT)
    top = res.astype(BF).astype(F32)
    mid = (res - top).astype(BF).astype(F32)
    low = res - top - mid
    pad = jnp.zeros((16, STK - 24), F32)
    for k in range(4):
        cut = slice(8 * k, 8 * (k + 1))
        out_refs[k][...] = jnp.concatenate([top[:, cut], mid[:, cut], low[:, cut], pad], axis=1).astype(BF)


def run(kernel, outs, scratch, args, near):
    space = [pltpu.VMEM if n else pltpu.HBM for n in near]
    return pl.pallas_call(
        kernel,
        out_shape=outs,
        in_specs=[pl.BlockSpec(memory_space=m) for m in space],
        scratch_shapes=scratch,
        compiler_params=pltpu.CompilerParams(vmem_limit_bytes=52 << 20),
    )(*[pltpu.with_memory_space_constraint(a, m) for a, m in zip(args, space)])


def like(a):
    return pltpu.VMEM(a.shape, a.dtype)


def stage_pack(*args):
    args = (*args, jnp.asarray(tables()["zf"]))
    npw = args[1].shape[1]
    return run(
        pack_kernel,
        pltpu.VMEM((OWN * MSG, STK), BF),
        [
            pltpu.VMEM((2 * W, npw), BF),
            pltpu.VMEM((512, npw), BF),
            pltpu.VMEM((DEP, OWN * 8, STK), F32),
            *map(like, args),
            pltpu.SemaphoreType.DMA((len(args),)),
        ],
        args,
        (0, 0, 0, 0),
    )


def stage_over(sub, prevs):
    return run(overlap_kernel, [pltpu.VMEM((16, STK), BF)] * 4, [], (sub, *prevs), (1, 1, 1, 1, 1))


def stage_plane(got, pot):
    args = [jnp.asarray(tables()[k]) for k in ("yf", "xf", "xi", "yi")]
    return run(
        plane_kernel,
        pltpu.VMEM((OWN * MSG, STK), BF),
        [
            pltpu.VMEM((OWN, W, STK), BF),
            pltpu.VMEM((OWN, STK), F32),
            pltpu.VMEM((ROWS * N, STK), F32),
            pltpu.VMEM((ROWS * N, STK), F32),
            like(pot),
            *map(like, args),
            pltpu.SemaphoreType.DMA((5,)),
        ],
        (got, pot, *args),
        (1, 0, 0, 0, 0, 0),
    )


def stage_wave(got, *args):
    args = (*args, jnp.asarray(tables()["zi"]))
    order = (args[0], args[1], args[2], args[3])
    return run(
        wave_kernel,
        (jax.ShapeDtypeStruct(args[0].shape, BF), jax.ShapeDtypeStruct((2, 4), F32)),
        [pltpu.VMEM((DEP, OWN * 8, STK), F32), *map(like, order), pltpu.SemaphoreType.DMA((len(args),))],
        (got, *order),
        (1, 0, 0, 0, 0),
    )


def exchange(tiles):
    return lax.all_to_all(tiles, "fft", 0, 0, tiled=True).reshape(OWN * MSG, STK)


TILES = (OWN, MSG // 2, 2, STK)


def per_device(orbitals, sphere_slot, stick_column, potential, subspace, previous):
    npw = sphere_slot.shape[0]
    slot = sphere_slot.reshape(1, npw)
    col = stick_column.reshape(1, STK)
    send = stage_pack(orbitals, slot, col)
    got = exchange(send.reshape(TILES))
    shifts = [[(g, (g + k) % 4) for g in range(4)] for k in (1, 2, 3)]
    others = [lax.ppermute(previous, "band", s) for s in shifts]
    over = stage_over(subspace, [previous, *others])
    mine = [over[0]] + [lax.ppermute(over[k], "band", [(b, a) for a, b in shifts[k - 1]]) for k in (1, 2, 3)]
    field = stage_plane(got, potential)
    sums = jnp.concatenate([jnp.stack(mine)] * 2)
    sums = lax.dynamic_slice_in_dim(sums, (4 - lax.axis_index("band")) % 4, 4, 0).reshape(OWN, 1, STK)
    head = jnp.pad(sums, ((0, 0), (0, 1), (0, 0)))[:, None]
    back = exchange(lax.dynamic_update_slice(field.reshape(TILES), head, (0, 0, 0, 0)))
    applied, total = stage_wave(back, orbitals, slot, col)
    return applied, total.reshape(2, 1, 4)


def solution(mesh):
    return jax.shard_map(
        per_device,
        mesh=mesh,
        in_specs=(
            P("band", None, "fft"),
            P("fft"),
            P("fft"),
            P("fft", None, None),
            P("band", None, "fft"),
            P("band", None, "fft"),
        ),
        out_specs=(P("band", None, "fft"), P(None, "fft", "band")),
        check_vma=False,
    )
```

```python
import functools
import math

import jax
import jax.numpy as jnp
import numpy as np
from jax import lax
from jax.experimental import pallas as pl
from jax.experimental.pallas import tpu as pltpu
from jax.sharding import PartitionSpec as P


BF = jnp.bfloat16
F32 = jnp.float32
N = 192
OWN = 64
DEP = N // OWN
STK = 128
W = 256
ROWS = 8 * DEP
EXT = 2
MSG = EXT + ROWS
GRP = 16
CUT = 512
NT = (((1,), (1,)), ((), ()))
TN = (((0,), (0,)), ((), ()))


def dot(a, b, dims=(((1,), (0,)), ((), ()))):
    return lax.dot_general(a, b, dims, preferred_element_type=F32)


@functools.cache
def tables():
    def trig(rows, cols, scale):
        angle = (np.outer(rows, cols) % N) * (2.0 * math.pi / N)
        return np.cos(angle) * scale, np.sin(angle) * scale

    nat = np.arange(N)
    dealt = (np.arange(DEP)[:, None] + DEP * np.arange(OWN)[None, :]).reshape(-1)

    def wide(a, rows, cols):
        out = np.zeros((rows, cols))
        out[: a.shape[0], : a.shape[1]] = a
        return out

    def left(rows, cols, scale, sign, width):
        c, s = trig(rows, cols, scale)
        c, s = wide(c, N, width), wide(s * sign, N, width)
        return np.block([[c, -s], [s, c]])

    def right(rows, cols, scale, sign, order, width):
        c, s = trig(rows, cols, scale)
        c, s = wide(c, N, width), wide(s * sign, N, width)
        full = np.block([[c, s], [-s, c]])
        return full if order is None else full[np.ix_(order, order)]

    packed = np.concatenate([np.arange(128), N + np.arange(128), np.arange(128, N), np.arange(N + 128, 2 * N)])
    inv = 1.0 / N
    out = {
        "zf": left(dealt, nat, 1.0, 1.0, W),
        "yf": right(nat, nat, 1.0, 1.0, packed, N),
        "xf": left(nat, dealt, 1.0, 1.0, N),
        "xi": left(dealt, nat, inv, -1.0, N),
        "yi": right(nat, nat, inv, -1.0, packed, N),
        "zi": right(dealt, nat, inv, -1.0, None, W),
    }
    return {k: v.astype(np.float32).astype(BF) for k, v in out.items()}


def iota(shape, dim):
    return lax.broadcasted_iota(jnp.int32, shape, dim)


def column_coords(col):
    c = col.astype(F32)
    x = jnp.floor((c + 0.5) * (1.0 / N))
    return x, c - x * N


def fetch(sems, *pairs):
    copies = [pltpu.make_async_copy(src, dst, sems.at[i]) for i, (src, dst) in enumerate(pairs)]
    for copy in copies:
        copy.start()
    return copies


def pack_kernel(
    orb_hbm, slot_hbm, col_hbm, zf_hbm, out_ref, a_scr, b_scr, m_scr, orb_ref, slot_ref, col_ref, zf_ref, sems
):
    copies = fetch(sems, (slot_hbm, slot_ref), (orb_hbm, orb_ref), (col_hbm, col_ref), (zf_hbm, zf_ref))
    npw = slot_ref.shape[1]
    copies[0].wait()
    slot = slot_ref[...]
    low = slot & 63
    high = ((slot >> 6) & 1) * W + (slot >> 7)
    half = 1024
    copies[1].wait()
    for i in range(0, npw, half):
        cut = slice(i, i + half)
        a_scr[:, cut] = jnp.where(iota((2 * W, half), 0) == high[:, cut], 1.0, 0.0).astype(BF)
        hit = iota((64, half), 0) == low[:, cut]
        for j in range(8):
            row = orb_ref[j // 2, j % 2 : j % 2 + 1, cut].astype(F32)
            b_scr[64 * j : 64 * (j + 1), cut] = jnp.where(hit, row, 0.0).astype(BF)
    grid = dot(b_scr[...], a_scr[...], NT).astype(BF)
    rows = []
    for b in range(4):
        for h in range(2):
            rows.append(
                jnp.concatenate(
                    [grid[64 * (2 * b + p) : 64 * (2 * b + p + 1), W * h : W * (h + 1)] for p in range(2)],
                    axis=1,
                )
            )
    stick = jnp.concatenate(rows, axis=0)
    copies[2].wait()
    copies[3].wait()
    wave = dot(zf_ref[...], stick, NT)
    x, y = column_coords(col_ref[...])
    xl = x - DEP * jnp.floor((x + 0.5) * (1.0 / DEP))
    ext = jnp.concatenate([xl, y], axis=0)
    for r in range(DEP):
        for j in range(8):
            base = (j % 2) * N + r * OWN
            m_scr[r, pl.ds(j, OWN, stride=8), :] = wave[base : base + OWN, STK * (j // 2) : STK * (j // 2 + 1)]

    def pour(i, carry):
        at = pl.multiple_of(i * GRP * 8, 8)
        block = [m_scr[r, pl.ds(at, GRP * 8), :] for r in range(DEP)]
        parts = []
        for u in range(GRP):
            parts += [ext] + [block[r][8 * u : 8 * u + 8] for r in range(DEP)]
        out_ref[pl.ds(pl.multiple_of(i * GRP * MSG, 16), GRP * MSG), :] = jnp.concatenate(parts, axis=0).astype(BF)
        return carry

    lax.fori_loop(0, OWN // GRP, pour, 0)


def plane_kernel(
    in_ref, ext_ref, pot_hbm, yf_hbm, xf_hbm, xi_hbm, yi_hbm, out_ref, oh_scr, xl_scr, lo_scr, hi_scr, pot_scr, yf, xf, xi, yi, sems
):
    rows = ROWS
    copies = fetch(sems, (yf_hbm, yf), (xf_hbm, xf), (pot_hbm, pot_scr), (xi_hbm, xi), (yi_hbm, yi))
    halves = (lo_scr, hi_scr)

    def scatter(i, carry):
        block = in_ref[pl.ds(pl.multiple_of(i * GRP * MSG, 16), GRP * MSG), :].astype(F32)
        for u in range(GRP):
            d = i * GRP + u
            m = block[MSG * u : MSG * (u + 1)]
            xl, y = m[0:1], m[1:2].astype(jnp.int32)
            xl_scr[pl.ds(d, 1), :] = xl
            hot = jnp.where(iota((N, STK), 0) == y, 1.0, 0.0).astype(BF)
            hot = jnp.concatenate([hot, hot[STK:]], axis=0)
            oh_scr[d] = hot
            lhs = jnp.concatenate([jnp.where(xl == k, m[EXT:], 0.0) for k in range(DEP)], axis=0).astype(BF)
            res = dot(lhs, hot, NT)
            for k in range(DEP):
                for r in range(DEP):
                    base = k * rows + r * 8
                    for h in range(2):
                        at = pl.multiple_of((r * N + k * OWN + d) * 8, 8)
                        halves[h][pl.ds(at, 8), :] = res[
                            base : base + 8, h * STK : (h + 1) * STK
                        ]
        return carry

    lax.fori_loop(0, OWN // GRP, scatter, 0)
    for copy in copies:
        copy.wait()

    left = iota((N, STK), 1) < STK // 2

    def mixed(one, two):
        return (
            jnp.where(left, one, pltpu.roll(two, STK // 2, 1)),
            jnp.where(left, pltpu.roll(one, STK // 2, 1), two),
        )

    def plane(r, carry):
        at = r * 8 * N
        lined = []
        for b in range(4):
            low = [lo_scr[pl.ds(at + 2 * b + p, N, stride=8), :] for p in range(2)]
            high = [hi_scr[pl.ds(at + 2 * b + p, N, stride=8), :] for p in range(2)]
            lined.append(jnp.concatenate([*low, jnp.where(left, *high)], axis=1).astype(BF))
        ay = dot(jnp.concatenate(lined, axis=0), yf[...]).reshape(4, N, 2 * N)
        blocks = [jnp.concatenate([ay[b, :, :STK], ay[b, :, STK : 2 * STK]], axis=0) for b in range(4)]
        for b in range(0, 4, 2):
            blocks.append(jnp.concatenate(mixed(ay[b, :, 2 * STK :], ay[b + 1, :, 2 * STK :]), axis=0))
        ax = dot(xf[...], jnp.concatenate(blocks, axis=1).astype(BF))
        pot = pot_scr[r]
        pot = jnp.concatenate([pot[:, :STK]] * 4 + [pot[:, STK:]] * 4, axis=1)
        pot = jnp.concatenate([pot, pot], axis=0)
        bx = dot(xi[...], (ax * pot).astype(BF))
        tails = []
        for b in range(0, 4, 2):
            cut = slice((4 + b // 2) * STK, (5 + b // 2) * STK)
            tails += mixed(bx[:N, cut], bx[N:, cut])
        lined = [
            jnp.concatenate([bx[:N, b * STK : (b + 1) * STK], bx[N:, b * STK : (b + 1) * STK], tails[b]], axis=1)
            for b in range(4)
        ]
        by = dot(jnp.concatenate(lined, axis=0).astype(BF), yi[...])
        for b in range(4):
            part = by[b * N : (b + 1) * N]
            high = part[:, 2 * STK :]
            for p in range(2):
                lo_scr[pl.ds(at + 2 * b + p, N, stride=8), :] = part[:, p * STK : (p + 1) * STK]
                hi_scr[pl.ds(at + 2 * b + p, N, stride=8), :] = jnp.where(left, *((high, 0.0) if p == 0 else (0.0, high)))
        return carry

    lax.fori_loop(0, DEP, plane, 0)

    def gather(i, carry):
        parts = []
        for u in range(GRP // 2):
            pair = [i * GRP + 2 * u, i * GRP + 2 * u + 1]
            blocks = []
            for d in pair:
                for k in range(DEP):
                    for r in range(DEP):
                        blocks.append(
                            jnp.concatenate(
                                [
                                    half[pl.ds(pl.multiple_of((r * N + k * OWN + d) * 8, 8), 8), :]
                                    for half in halves
                                ],
                                axis=1,
                            )
                        )
            lhs = jnp.concatenate(blocks, axis=0).astype(BF)
            res = dot(lhs, jnp.concatenate([oh_scr[d] for d in pair], axis=1))
            for t, d in enumerate(pair):
                xl = xl_scr[pl.ds(d, 1), :]
                took = [
                    res[(t * DEP + k) * rows : (t * DEP + k + 1) * rows, t * STK : (t + 1) * STK] for k in range(DEP)
                ]
                field = jnp.where(xl == 0.0, took[0], jnp.where(xl == 1.0, took[1], took[2]))
                parts += [ext_ref[pl.ds(d, 1), :], jnp.zeros((EXT - 1, STK), F32), field]
        out_ref[pl.ds(pl.multiple_of(i * GRP * MSG, 16), GRP * MSG), :] = jnp.concatenate(parts, axis=0).astype(BF)
        return carry

    lax.fori_loop(0, OWN // GRP, gather, 0)


def ready_kernel(
    orb_hbm, slot_hbm, col_hbm, zi_hbm, hot_ref, base_ref, slot_ref, zi_ref, orb_ref, col_ref, sems
):
    copies = fetch(sems, (slot_hbm, slot_ref), (orb_hbm, orb_ref), (col_hbm, col_ref), (zi_hbm, zi_ref))
    for copy in copies:
        copy.wait()
    x, y = column_coords(col_ref[...])
    x = jnp.where(x >= N // 2, x - N, x)
    y = jnp.where(y >= N // 2, y - N, y)
    square = x * x + y * y
    square = jnp.sum(jnp.where(iota((STK, STK), 0) == iota((STK, STK), 1), square, 0.0), axis=1, keepdims=True)

    def step(i, carry):
        cut = pl.ds(pl.multiple_of(i * CUT, CUT), CUT)
        slot = slot_ref[:, cut]
        z, stick = slot >> 7, slot & (STK - 1)
        hot_ref[:, cut] = jnp.where(iota((N, CUT), 0) == z, 1.0, 0.0).astype(BF)
        fz = jnp.where(z >= N // 2, z - N, z).astype(F32)
        flat = jnp.sum(jnp.where(iota((STK, CUT), 0) == stick, square, 0.0), axis=0, keepdims=True)
        kinetic = (fz * fz + flat) * (2.0 / (N * N))
        for b in range(4):
            base_ref[b, :, cut] = kinetic * orb_ref[b, :, cut].astype(F32)
        return carry

    lax.fori_loop(0, hot_ref.shape[1] // CUT, step, 0)


def wave_kernel(in_ref, hot_ref, base_ref, slot_ref, zi_ref, out_ref, sum_ref, m_scr):
    npw = slot_ref.shape[1]

    def unpour(i, total):
        block = in_ref[pl.ds(pl.multiple_of(i * GRP * MSG, 16), GRP * MSG), :].astype(F32)
        for u in range(GRP):
            total = total + block[MSG * u : MSG * u + 1]
            for r in range(DEP):
                row = MSG * u + EXT + 8 * r
                m_scr[r, pl.ds(pl.multiple_of((i * GRP + u) * 8, 8), 8), :] = block[row : row + 8]
        return total

    total = lax.fori_loop(0, OWN // GRP, unpour, jnp.zeros((1, STK), F32))
    total = total[:, 0:8] + total[:, 8:16] + total[:, 16:24]
    sum_ref[...] = jnp.concatenate([total[:, 0:4], total[:, 4:8]], axis=0)
    cols = []
    for b in range(4):
        picks = [m_scr[r, pl.ds(2 * b + p, OWN, stride=8), :] for p in range(2) for r in range(DEP)]
        cols.append(jnp.concatenate(picks, axis=0))
    spectrum = jnp.concatenate(cols, axis=1).astype(BF)
    sticks = dot(spectrum, zi_ref[...], TN).astype(BF)

    def pick(i, carry):
        cut = pl.ds(pl.multiple_of(i * CUT, CUT), CUT)
        hit = iota((STK, CUT), 0) == (slot_ref[:, cut] & (STK - 1))
        hot = hot_ref[:, cut]
        lines = []
        for p in range(2):
            res = dot(sticks[:, p * W : p * W + N], hot)
            lines.append(
                [jnp.sum(jnp.where(hit, res[b * STK : (b + 1) * STK], 0.0), axis=0, keepdims=True) for b in range(4)]
            )
        for b in range(4):
            done = jnp.concatenate([lines[0][b], lines[1][b]], axis=0) + base_ref[b, :, cut]
            out_ref[b, :, cut] = done.astype(BF)
        return carry

    lax.fori_loop(0, npw // CUT, pick, 0, unroll=2)


def overlap_kernel(sub_ref, *refs):
    refs, out_refs = refs[:4], refs[4:]
    sub = sub_ref[...].astype(F32)
    sub = jnp.concatenate([sub[:, 0], sub[:, 1]], axis=1).astype(BF)
    rows = []
    for ref in refs:
        prev = ref[...].astype(F32)
        re, im = prev[:, 0], prev[:, 1]
        rows.append(jnp.concatenate([re, im], axis=1))
        rows.append(jnp.concatenate([im, -re], axis=1))
    res = dot(sub, jnp.concatenate(rows, axis=0).astype(BF), NT)
    top = res.astype(BF).astype(F32)
    mid = (res - top).astype(BF).astype(F32)
    low = res - top - mid
    pad = jnp.zeros((16, STK - 24), F32)
    for k in range(4):
        cut = slice(8 * k, 8 * (k + 1))
        out_refs[k][...] = jnp.concatenate([top[:, cut], mid[:, cut], low[:, cut], pad], axis=1).astype(BF)


def run(kernel, outs, scratch, args, near, room):
    space = [pltpu.VMEM if n else pltpu.HBM for n in near]
    return pl.pallas_call(
        kernel,
        out_shape=outs,
        in_specs=[pl.BlockSpec(memory_space=m) for m in space],
        scratch_shapes=scratch,
        compiler_params=pltpu.CompilerParams(vmem_limit_bytes=room << 20),
    )(*[pltpu.with_memory_space_constraint(a, m) for a, m in zip(args, space)])


def like(a):
    return pltpu.VMEM(a.shape, a.dtype)


def stage_pack(*args):
    args = (*args, jnp.asarray(tables()["zf"]))
    npw = args[1].shape[1]
    return run(
        pack_kernel,
        pltpu.VMEM((OWN * MSG, STK), BF),
        [
            pltpu.VMEM((2 * W, npw), BF),
            pltpu.VMEM((512, npw), BF),
            pltpu.VMEM((DEP, OWN * 8, STK), F32),
            *map(like, args),
            pltpu.SemaphoreType.DMA((len(args),)),
        ],
        args,
        (0, 0, 0, 0),
        24,
    )


def stage_over(sub, prevs):
    return run(overlap_kernel, [pltpu.VMEM((16, STK), BF)] * 4, [], (sub, *prevs), (1, 1, 1, 1, 1), 8)


def stage_plane(got, ext, pot):
    args = [jnp.asarray(tables()[k]) for k in ("yf", "xf", "xi", "yi")]
    return run(
        plane_kernel,
        pltpu.VMEM((OWN * MSG, STK), BF),
        [
            pltpu.VMEM((OWN, W, STK), BF),
            pltpu.VMEM((OWN, STK), F32),
            pltpu.VMEM((ROWS * N, STK), F32),
            pltpu.VMEM((ROWS * N, STK), F32),
            like(pot),
            *map(like, args),
            pltpu.SemaphoreType.DMA((5,)),
        ],
        (got, ext, pot, *args),
        (1, 1, 0, 0, 0, 0, 0),
        32,
    )


def stage_ready(orb, slot, col):
    args = (orb, slot, col, jnp.asarray(tables()["zi"]))
    return run(
        ready_kernel,
        [pltpu.VMEM((N, slot.shape[1]), BF), pltpu.VMEM(orb.shape, F32), like(slot), like(args[3])],
        [like(orb), like(col), pltpu.SemaphoreType.DMA((4,))],
        args,
        (0, 0, 0, 0),
        12,
    )


def stage_wave(got, hot, base, slot, zi):
    return run(
        wave_kernel,
        (jax.ShapeDtypeStruct(base.shape, BF), jax.ShapeDtypeStruct((2, 4), F32)),
        [pltpu.VMEM((DEP, OWN * 8, STK), F32)],
        (got, hot, base, slot, zi),
        (1, 1, 1, 1, 1),
        16,
    )


def exchange(tiles):
    return lax.all_to_all(tiles, "fft", 0, 0, tiled=True).reshape(OWN * MSG, STK)


TILES = (OWN, MSG // 2, 2, STK)


def per_device(orbitals, sphere_slot, stick_column, potential, subspace, previous):
    npw = sphere_slot.shape[0]
    slot = sphere_slot.reshape(1, npw)
    col = stick_column.reshape(1, STK)
    shifts = [[(g, (g + k) % 4) for g in range(4)] for k in (1, 2, 3)]
    others = [lax.ppermute(previous, "band", s) for s in shifts]
    send = stage_pack(orbitals, slot, col)
    got = exchange(send.reshape(TILES))
    over = stage_over(subspace, [previous, *others])
    mine = [over[0]] + [lax.ppermute(over[k], "band", [(b, a) for a, b in shifts[k - 1]]) for k in (1, 2, 3)]
    sums = jnp.concatenate([jnp.stack(mine)] * 2)
    sums = lax.dynamic_slice_in_dim(sums, (4 - lax.axis_index("band")) % 4, 4, 0).reshape(OWN, STK)
    prepared = stage_ready(orbitals, slot, col)
    field = stage_plane(got, sums.astype(F32), potential)
    back = exchange(field.reshape(TILES))
    applied, total = stage_wave(back, *prepared)
    return applied, total.reshape(2, 1, 4)


def solution(mesh):
    return jax.shard_map(
        per_device,
        mesh=mesh,
        in_specs=(
            P("band", None, "fft"),
            P("fft"),
            P("fft"),
            P("fft", None, None),
            P("band", None, "fft"),
            P("band", None, "fft"),
        ),
        out_specs=(P("band", None, "fft"), P(None, "fft", "band")),
        check_vma=False,
    )
```

```python
import functools
import math

import jax
import jax.numpy as jnp
import numpy as np
from jax import lax
from jax.experimental import pallas as pl
from jax.experimental.pallas import tpu as pltpu
from jax.sharding import PartitionSpec as P


BF = jnp.bfloat16
F32 = jnp.float32
N = 192
OWN = 64
DEP = N // OWN
STK = 128
W = 256
ROWS = 8 * DEP
EXT = 2
MSG = EXT + ROWS
GRP = 16
CUT = 512
NT = (((1,), (1,)), ((), ()))
TN = (((0,), (0,)), ((), ()))


def dot(a, b, dims=(((1,), (0,)), ((), ()))):
    return lax.dot_general(a, b, dims, preferred_element_type=F32)


@functools.cache
def tables():
    def trig(rows, cols, scale):
        angle = (np.outer(rows, cols) % N) * (2.0 * math.pi / N)
        return np.cos(angle) * scale, np.sin(angle) * scale

    nat = np.arange(N)
    dealt = (np.arange(DEP)[:, None] + DEP * np.arange(OWN)[None, :]).reshape(-1)

    def wide(a, rows, cols):
        out = np.zeros((rows, cols))
        out[: a.shape[0], : a.shape[1]] = a
        return out

    def left(rows, cols, scale, sign, width):
        c, s = trig(rows, cols, scale)
        c, s = wide(c, N, width), wide(s * sign, N, width)
        return np.block([[c, -s], [s, c]])

    def right(rows, cols, scale, sign, order, width):
        c, s = trig(rows, cols, scale)
        c, s = wide(c, N, width), wide(s * sign, N, width)
        full = np.block([[c, s], [-s, c]])
        return full if order is None else full[np.ix_(order, order)]

    packed = np.concatenate([np.arange(128), N + np.arange(128), np.arange(128, N), np.arange(N + 128, 2 * N)])
    inv = 1.0 / N
    out = {
        "zf": left(dealt, nat, 1.0, 1.0, W),
        "yf": right(nat, nat, 1.0, 1.0, packed, N),
        "xf": left(nat, dealt, 1.0, 1.0, N),
        "xi": left(dealt, nat, inv, -1.0, N),
        "yi": right(nat, nat, inv, -1.0, packed, N),
        "zi": right(dealt, nat, inv, -1.0, None, W),
    }
    return {k: v.astype(np.float32).astype(BF) for k, v in out.items()}


def iota(shape, dim):
    return lax.broadcasted_iota(jnp.int32, shape, dim)


def column_coords(col):
    c = col.astype(F32)
    x = jnp.floor((c + 0.5) * (1.0 / N))
    return x, c - x * N


def fetch(sems, *pairs):
    copies = [pltpu.make_async_copy(src, dst, sems.at[i]) for i, (src, dst) in enumerate(pairs)]
    for copy in copies:
        copy.start()
    return copies


def pack_kernel(
    orb_hbm, slot_hbm, col_hbm, zf_hbm, out_hbm, a_scr, b_scr, m_scr, out_ref, orb_ref, slot_ref, col_ref, zf_ref, sems
):
    copies = fetch(sems, (slot_hbm, slot_ref), (orb_hbm, orb_ref), (col_hbm, col_ref), (zf_hbm, zf_ref))
    npw = slot_ref.shape[1]
    copies[0].wait()
    slot = slot_ref[...]
    low = slot & 63
    high = ((slot >> 6) & 1) * W + (slot >> 7)
    half = 1024
    copies[1].wait()
    for i in range(0, npw, half):
        cut = slice(i, i + half)
        a_scr[:, cut] = jnp.where(iota((2 * W, half), 0) == high[:, cut], 1.0, 0.0).astype(BF)
        hit = iota((64, half), 0) == low[:, cut]
        for j in range(8):
            row = orb_ref[j // 2, j % 2 : j % 2 + 1, cut].astype(F32)
            b_scr[64 * j : 64 * (j + 1), cut] = jnp.where(hit, row, 0.0).astype(BF)
    grid = dot(b_scr[...], a_scr[...], NT).astype(BF)
    rows = []
    for b in range(4):
        for h in range(2):
            rows.append(
                jnp.concatenate(
                    [grid[64 * (2 * b + p) : 64 * (2 * b + p + 1), W * h : W * (h + 1)] for p in range(2)],
                    axis=1,
                )
            )
    stick = jnp.concatenate(rows, axis=0)
    copies[2].wait()
    copies[3].wait()
    wave = dot(zf_ref[...], stick, NT)
    x, y = column_coords(col_ref[...])
    xl = x - DEP * jnp.floor((x + 0.5) * (1.0 / DEP))
    ext = jnp.concatenate([xl, y], axis=0)
    for r in range(DEP):
        for j in range(8):
            base = (j % 2) * N + r * OWN
            m_scr[r, pl.ds(j, OWN, stride=8), :] = wave[base : base + OWN, STK * (j // 2) : STK * (j // 2 + 1)]

    copies = []
    for i in range(OWN // GRP):
        parts = []
        for u in range(i * GRP, (i + 1) * GRP):
            parts += [ext] + [m_scr[r, 8 * u : 8 * u + 8] for r in range(DEP)]
        cut = pl.ds(i * GRP * MSG, GRP * MSG)
        out_ref[cut, :] = jnp.concatenate(parts, axis=0).astype(BF)
        copies.append(pltpu.make_async_copy(out_ref.at[cut], out_hbm.at[cut], sems.at[4 + i]))
        copies[-1].start()
    for copy in copies:
        copy.wait()


def plane_kernel(
    in_ref, pot_hbm, yf_hbm, xf_hbm, xi_hbm, yi_hbm, out_ref, oh_scr, xl_scr, lo_scr, hi_scr, pot_scr, yf, xf, xi, yi, sems
):
    rows = ROWS
    copies = fetch(sems, (yf_hbm, yf), (xf_hbm, xf), (pot_hbm, pot_scr), (xi_hbm, xi), (yi_hbm, yi))
    halves = (lo_scr, hi_scr)

    def scatter(i, carry):
        block = in_ref[pl.ds(pl.multiple_of(i * GRP * MSG, 16), GRP * MSG), :].astype(F32)
        for u in range(GRP):
            d = i * GRP + u
            m = block[MSG * u : MSG * (u + 1)]
            xl, y = m[0:1], m[1:2].astype(jnp.int32)
            xl_scr[pl.ds(d, 1), :] = xl
            hot = jnp.where(iota((N, STK), 0) == y, 1.0, 0.0).astype(BF)
            hot = jnp.concatenate([hot, hot[STK:]], axis=0)
            oh_scr[d] = hot
            lhs = jnp.concatenate([jnp.where(xl == k, m[EXT:], 0.0) for k in range(DEP)], axis=0).astype(BF)
            res = dot(lhs, hot, NT)
            for k in range(DEP):
                for r in range(DEP):
                    base = k * rows + r * 8
                    for h in range(2):
                        at = pl.multiple_of((r * N + k * OWN + d) * 8, 8)
                        halves[h][pl.ds(at, 8), :] = res[
                            base : base + 8, h * STK : (h + 1) * STK
                        ]
        return carry

    lax.fori_loop(0, OWN // GRP, scatter, 0)
    for copy in copies:
        copy.wait()

    left = iota((N, STK), 1) < STK // 2

    def mixed(one, two):
        return (
            jnp.where(left, one, pltpu.roll(two, STK // 2, 1)),
            jnp.where(left, pltpu.roll(one, STK // 2, 1), two),
        )

    def plane(r, carry):
        at = r * 8 * N
        lined = []
        for b in range(4):
            low = [lo_scr[pl.ds(at + 2 * b + p, N, stride=8), :] for p in range(2)]
            high = [hi_scr[pl.ds(at + 2 * b + p, N, stride=8), :] for p in range(2)]
            lined.append(jnp.concatenate([*low, jnp.where(left, *high)], axis=1).astype(BF))
        ay = dot(jnp.concatenate(lined, axis=0), yf[...]).reshape(4, N, 2 * N)
        blocks = [jnp.concatenate([ay[b, :, :STK], ay[b, :, STK : 2 * STK]], axis=0) for b in range(4)]
        for b in range(0, 4, 2):
            blocks.append(jnp.concatenate(mixed(ay[b, :, 2 * STK :], ay[b + 1, :, 2 * STK :]), axis=0))
        ax = dot(xf[...], jnp.concatenate(blocks, axis=1).astype(BF))
        pot = pot_scr[r]
        pot = jnp.concatenate([pot[:, :STK]] * 4 + [pot[:, STK:]] * 4, axis=1)
        pot = jnp.concatenate([pot, pot], axis=0)
        bx = dot(xi[...], (ax * pot).astype(BF))
        tails = []
        for b in range(0, 4, 2):
            cut = slice((4 + b // 2) * STK, (5 + b // 2) * STK)
            tails += mixed(bx[:N, cut], bx[N:, cut])
        lined = [
            jnp.concatenate([bx[:N, b * STK : (b + 1) * STK], bx[N:, b * STK : (b + 1) * STK], tails[b]], axis=1)
            for b in range(4)
        ]
        by = dot(jnp.concatenate(lined, axis=0).astype(BF), yi[...])
        for b in range(4):
            part = by[b * N : (b + 1) * N]
            high = part[:, 2 * STK :]
            for p in range(2):
                lo_scr[pl.ds(at + 2 * b + p, N, stride=8), :] = part[:, p * STK : (p + 1) * STK]
                hi_scr[pl.ds(at + 2 * b + p, N, stride=8), :] = jnp.where(left, *((high, 0.0) if p == 0 else (0.0, high)))
        return carry

    lax.fori_loop(0, DEP, plane, 0)

    def gather(i, carry):
        parts = []
        for u in range(GRP // 2):
            pair = [i * GRP + 2 * u, i * GRP + 2 * u + 1]
            blocks = []
            for d in pair:
                for k in range(DEP):
                    for r in range(DEP):
                        blocks.append(
                            jnp.concatenate(
                                [
                                    half[pl.ds(pl.multiple_of((r * N + k * OWN + d) * 8, 8), 8), :]
                                    for half in halves
                                ],
                                axis=1,
                            )
                        )
            lhs = jnp.concatenate(blocks, axis=0).astype(BF)
            res = dot(lhs, jnp.concatenate([oh_scr[d] for d in pair], axis=1))
            for t, d in enumerate(pair):
                xl = xl_scr[pl.ds(d, 1), :]
                took = [
                    res[(t * DEP + k) * rows : (t * DEP + k + 1) * rows, t * STK : (t + 1) * STK] for k in range(DEP)
                ]
                field = jnp.where(xl == 0.0, took[0], jnp.where(xl == 1.0, took[1], took[2]))
                parts += [jnp.zeros((EXT, STK), F32), field]
        out_ref[pl.ds(pl.multiple_of(i * GRP * MSG, 16), GRP * MSG), :] = jnp.concatenate(parts, axis=0).astype(BF)
        return carry

    lax.fori_loop(0, OWN // GRP, gather, 0)


def ready_kernel(
    orb_hbm, slot_hbm, col_hbm, zi_hbm, hot_ref, base_ref, slot_ref, zi_ref, orb_ref, col_ref, sems
):
    copies = fetch(sems, (slot_hbm, slot_ref), (orb_hbm, orb_ref), (col_hbm, col_ref), (zi_hbm, zi_ref))
    for copy in copies:
        copy.wait()
    x, y = column_coords(col_ref[...])
    x = jnp.where(x >= N // 2, x - N, x)
    y = jnp.where(y >= N // 2, y - N, y)
    square = x * x + y * y
    square = jnp.sum(jnp.where(iota((STK, STK), 0) == iota((STK, STK), 1), square, 0.0), axis=1, keepdims=True)

    def step(i, carry):
        cut = pl.ds(pl.multiple_of(i * CUT, CUT), CUT)
        slot = slot_ref[:, cut]
        z, stick = slot >> 7, slot & (STK - 1)
        hot_ref[:, cut] = jnp.where(iota((N, CUT), 0) == z, 1.0, 0.0).astype(BF)
        fz = jnp.where(z >= N // 2, z - N, z).astype(F32)
        flat = jnp.sum(jnp.where(iota((STK, CUT), 0) == stick, square, 0.0), axis=0, keepdims=True)
        kinetic = (fz * fz + flat) * (2.0 / (N * N))
        for b in range(4):
            base_ref[b, :, cut] = kinetic * orb_ref[b, :, cut].astype(F32)
        return carry

    lax.fori_loop(0, hot_ref.shape[1] // CUT, step, 0)


def wave_kernel(in_ref, hot_ref, base_ref, slot_ref, zi_ref, out_ref, sum_ref, m_scr):
    npw = slot_ref.shape[1]

    def unpour(i, total):
        block = in_ref[pl.ds(pl.multiple_of(i * GRP * MSG, 16), GRP * MSG), :].astype(F32)
        for u in range(GRP):
            total = total + block[MSG * u : MSG * u + 1]
            for r in range(DEP):
                row = MSG * u + EXT + 8 * r
                m_scr[r, pl.ds(pl.multiple_of((i * GRP + u) * 8, 8), 8), :] = block[row : row + 8]
        return total

    total = lax.fori_loop(0, OWN // GRP, unpour, jnp.zeros((1, STK), F32))
    total = total[:, 0:8] + total[:, 8:16] + total[:, 16:24]
    sum_ref[...] = jnp.concatenate([total[:, 0:4], total[:, 4:8]], axis=0)
    cols = []
    for b in range(4):
        picks = [m_scr[r, pl.ds(2 * b + p, OWN, stride=8), :] for p in range(2) for r in range(DEP)]
        cols.append(jnp.concatenate(picks, axis=0))
    spectrum = jnp.concatenate(cols, axis=1).astype(BF)
    sticks = dot(spectrum, zi_ref[...], TN).astype(BF)

    def pick(i, carry):
        cut = pl.ds(pl.multiple_of(i * CUT, CUT), CUT)
        hit = iota((STK, CUT), 0) == (slot_ref[:, cut] & (STK - 1))
        hot = hot_ref[:, cut]
        lines = []
        for p in range(2):
            res = dot(sticks[:, p * W : p * W + N], hot)
            lines.append(
                [jnp.sum(jnp.where(hit, res[b * STK : (b + 1) * STK], 0.0), axis=0, keepdims=True) for b in range(4)]
            )
        for b in range(4):
            done = jnp.concatenate([lines[0][b], lines[1][b]], axis=0) + base_ref[b, :, cut]
            out_ref[b, :, cut] = done.astype(BF)
        return carry

    lax.fori_loop(0, npw // CUT, pick, 0, unroll=2)


def overlap_kernel(sub_ref, *refs):
    refs, out_refs = refs[:4], refs[4:]
    sub = sub_ref[...].astype(F32)
    sub = jnp.concatenate([sub[:, 0], sub[:, 1]], axis=1).astype(BF)
    rows = []
    for ref in refs:
        prev = ref[...].astype(F32)
        re, im = prev[:, 0], prev[:, 1]
        rows.append(jnp.concatenate([re, im], axis=1))
        rows.append(jnp.concatenate([im, -re], axis=1))
    res = dot(sub, jnp.concatenate(rows, axis=0).astype(BF), NT)
    top = res.astype(BF).astype(F32)
    mid = (res - top).astype(BF).astype(F32)
    low = res - top - mid
    pad = jnp.zeros((16, STK - 24), F32)
    for k in range(4):
        cut = slice(8 * k, 8 * (k + 1))
        out_refs[k][...] = jnp.concatenate([top[:, cut], mid[:, cut], low[:, cut], pad], axis=1).astype(BF)


def run(kernel, outs, scratch, args, near, room, to=None):
    space = [pltpu.VMEM if n else pltpu.HBM for n in near]
    return pl.pallas_call(
        kernel,
        out_shape=outs,
        in_specs=[pl.BlockSpec(memory_space=m) for m in space],
        **({} if to is None else {"out_specs": pl.BlockSpec(memory_space=to)}),
        scratch_shapes=scratch,
        compiler_params=pltpu.CompilerParams(vmem_limit_bytes=room << 20),
    )(*[pltpu.with_memory_space_constraint(a, m) for a, m in zip(args, space)])


def like(a):
    return pltpu.VMEM(a.shape, a.dtype)


def stage_pack(*args):
    args = (*args, jnp.asarray(tables()["zf"]))
    npw = args[1].shape[1]
    return run(
        pack_kernel,
        pltpu.HBM((OWN * MSG, STK), BF),
        [
            pltpu.VMEM((2 * W, npw), BF),
            pltpu.VMEM((512, npw), BF),
            pltpu.VMEM((DEP, OWN * 8, STK), F32),
            pltpu.VMEM((OWN * MSG, STK), BF),
            *map(like, args),
            pltpu.SemaphoreType.DMA((4 + OWN // GRP,)),
        ],
        args,
        (0, 0, 0, 0),
        24,
        pltpu.HBM,
    )


def stage_over(sub, prevs):
    return run(overlap_kernel, [pltpu.VMEM((16, STK), BF)] * 4, [], (sub, *prevs), (1, 1, 1, 1, 1), 8)


def stage_plane(got, pot):
    args = [jnp.asarray(tables()[k]) for k in ("yf", "xf", "xi", "yi")]
    return run(
        plane_kernel,
        pltpu.VMEM((OWN * MSG, STK), BF),
        [
            pltpu.VMEM((OWN, W, STK), BF),
            pltpu.VMEM((OWN, STK), F32),
            pltpu.VMEM((ROWS * N, STK), F32),
            pltpu.VMEM((ROWS * N, STK), F32),
            like(pot),
            *map(like, args),
            pltpu.SemaphoreType.DMA((5,)),
        ],
        (got, pot, *args),
        (1, 0, 0, 0, 0, 0),
        32,
    )


def stage_ready(orb, slot, col):
    args = (orb, slot, col, jnp.asarray(tables()["zi"]))
    return run(
        ready_kernel,
        [pltpu.VMEM((N, slot.shape[1]), BF), pltpu.VMEM(orb.shape, F32), like(slot), like(args[3])],
        [like(orb), like(col), pltpu.SemaphoreType.DMA((4,))],
        args,
        (0, 0, 0, 0),
        12,
    )


def stage_wave(got, hot, base, slot, zi):
    return run(
        wave_kernel,
        (jax.ShapeDtypeStruct(base.shape, BF), jax.ShapeDtypeStruct((2, 4), F32)),
        [pltpu.VMEM((DEP, OWN * 8, STK), F32)],
        (got, hot, base, slot, zi),
        (1, 1, 1, 1, 1),
        16,
    )


def exchange(tiles):
    return lax.all_to_all(tiles, "fft", 0, 0, tiled=True).reshape(OWN * MSG, STK)


TILES = (OWN, MSG // 2, 2, STK)


def per_device(orbitals, sphere_slot, stick_column, potential, subspace, previous):
    npw = sphere_slot.shape[0]
    slot = sphere_slot.reshape(1, npw)
    col = stick_column.reshape(1, STK)

    def swapped(a, k):
        return lax.ppermute(a, "band", [(g, g ^ k) for g in range(4)])

    beside = swapped(previous, 1)
    send = stage_pack(orbitals, slot, col)
    got = exchange(send.reshape(TILES))
    others = [beside, swapped(previous, 2), swapped(beside, 2)]
    over = stage_over(subspace, [previous, *others])
    mine = [over[0]] + [swapped(over[k], k) for k in (1, 2, 3)]
    prepared = stage_ready(orbitals, slot, col)
    field = stage_plane(got, potential)
    group = lax.axis_index("band")
    for k in (1, 2):
        mine = [jnp.where((group & k) > 0, mine[i ^ k], mine[i]) for i in range(4)]
    sums = jnp.concatenate(mine, axis=0).reshape(OWN, 1, 1, STK)
    head = jnp.pad(sums, ((0, 0), (0, 0), (0, EXT - 1), (0, 0)))
    back = exchange(lax.dynamic_update_slice(field.reshape(TILES), head, (0, 0, 0, 0)))
    applied, total = stage_wave(back, *prepared)
    return applied, total.reshape(2, 1, 4)


def solution(mesh):
    return jax.shard_map(
        per_device,
        mesh=mesh,
        in_specs=(
            P("band", None, "fft"),
            P("fft"),
            P("fft"),
            P("fft", None, None),
            P("band", None, "fft"),
            P("band", None, "fft"),
        ),
        out_specs=(P("band", None, "fft"), P(None, "fft", "band")),
        check_vma=False,
    )
```

```python
import functools
import math

import jax
import jax.numpy as jnp
import numpy as np
from jax import lax
from jax.experimental import pallas as pl
from jax.experimental.pallas import tpu as pltpu
from jax.sharding import PartitionSpec as P


BF = jnp.bfloat16
F32 = jnp.float32
N = 192
OWN = 64
DEP = N // OWN
STK = 128
W = 256
ROWS = 8 * DEP
EXT = 2
MSG = EXT + ROWS
GRP = 16
CUT = 512
NT = (((1,), (1,)), ((), ()))


def dot(a, b, dims=(((1,), (0,)), ((), ()))):
    return lax.dot_general(a, b, dims, preferred_element_type=F32)


@functools.cache
def tables():
    def trig(rows, cols, scale):
        angle = (np.outer(rows, cols) % N) * (2.0 * math.pi / N)
        return np.cos(angle) * scale, np.sin(angle) * scale

    nat = np.arange(N)
    dealt = (np.arange(DEP)[:, None] + DEP * np.arange(OWN)[None, :]).reshape(-1)

    half = nat[: N // 2]
    even, odd = (
        np.concatenate([part + DEP * (2 * np.arange(OWN // 2) + (part + q) % 2) for part in range(DEP)]) for q in range(2)
    )
    assert not (even % 2).any() and (odd % 2).all()

    def wide(a, rows, cols):
        out = np.zeros((rows, cols))
        out[: a.shape[0], : a.shape[1]] = a
        return out

    def left(rows, cols, scale, sign, width):
        c, s = trig(rows, cols, scale)
        c, s = wide(c, len(rows), width), wide(s * sign, len(rows), width)
        return np.block([[c, -s], [s, c]])

    def right(rows, cols, scale, sign, order, width):
        c, s = trig(rows, cols, scale)
        c, s = wide(c, N, width), wide(s * sign, N, width)
        full = np.block([[c, s], [-s, c]])
        return full if order is None else full[np.ix_(order, order)]

    packed = np.concatenate([np.arange(128), N + np.arange(128), np.arange(128, N), np.arange(N + 128, 2 * N)])
    by_block = np.arange(2 * N).reshape(2, DEP, 64).transpose(1, 0, 2).reshape(-1)
    inv = 1.0 / N
    out = {
        "zf": left(dealt, nat, 1.0, 1.0, N)[:, by_block],
        "yf": right(nat, nat, 1.0, 1.0, packed, N),
        "xe": left(half, even, 1.0, 1.0, N // 2),
        "xo": left(half, odd, 1.0, 1.0, N // 2),
        "ie": left(even, half, inv, -1.0, N // 2),
        "io": left(odd, half, inv, -1.0, N // 2),
        "yi": right(nat, nat, inv, -1.0, packed, N),
        "zi": left(np.concatenate([nat[::2], nat[1::2]]), dealt, inv, -1.0, N),
    }
    return {k: v.astype(np.float32).astype(BF) for k, v in out.items()}


def iota(shape, dim):
    return lax.broadcasted_iota(jnp.int32, shape, dim)


def column_coords(col):
    c = col.astype(F32)
    x = jnp.floor((c + 0.5) * (1.0 / N))
    return x, c - x * N


def fetch(sems, *pairs):
    copies = [pltpu.make_async_copy(src, dst, sems.at[i]) for i, (src, dst) in enumerate(pairs)]
    for copy in copies:
        copy.start()
    return copies


def pack_kernel(
    orb_hbm, slot_hbm, col_hbm, zf_hbm, out_hbm, a_scr, b_scr, m_scr, out_ref, orb_ref, slot_ref, col_ref, zf_ref, sems
):
    copies = fetch(sems, (slot_hbm, slot_ref), (orb_hbm, orb_ref), (col_hbm, col_ref), (zf_hbm, zf_ref))
    npw = slot_ref.shape[1]
    copies[0].wait()
    slot = slot_ref[...]
    low = (slot >> 7) & 63
    high = (slot >> 13) * STK + (slot & (STK - 1))
    half = 1024
    copies[1].wait()
    for i in range(0, npw, half):
        cut = slice(i, i + half)
        a_scr[:, cut] = jnp.where(iota((DEP * STK, half), 0) == high[:, cut], 1.0, 0.0).astype(BF)
        hit = iota((64, half), 0) == low[:, cut]
        for j in range(8):
            row = orb_ref[j // 2, j % 2 : j % 2 + 1, cut].astype(F32)
            b_scr[64 * j : 64 * (j + 1), cut] = jnp.where(hit, row, 0.0).astype(BF)
    grid = dot(a_scr[...], b_scr[...], NT).astype(BF)
    stick = jnp.concatenate(
        [
            jnp.concatenate([grid[STK * h : STK * (h + 1), STK * b : STK * (b + 1)] for h in range(DEP)], axis=1)
            for b in range(4)
        ],
        axis=0,
    )
    copies[2].wait()
    copies[3].wait()
    wave = dot(zf_ref[...], stick, NT)
    x, y = column_coords(col_ref[...])
    xl = x - DEP * jnp.floor((x + 0.5) * (1.0 / DEP))
    ext = jnp.concatenate([xl, y], axis=0)
    for r in range(DEP):
        for j in range(8):
            base = (j % 2) * N + r * OWN
            m_scr[r, pl.ds(j, OWN, stride=8), :] = wave[base : base + OWN, STK * (j // 2) : STK * (j // 2 + 1)]

    copies = []
    for i in range(OWN // GRP):
        parts = []
        for u in range(i * GRP, (i + 1) * GRP):
            parts += [ext] + [m_scr[r, 8 * u : 8 * u + 8] for r in range(DEP)]
        cut = pl.ds(i * GRP * MSG, GRP * MSG)
        out_ref[cut, :] = jnp.concatenate(parts, axis=0).astype(BF)
        copies.append(pltpu.make_async_copy(out_ref.at[cut], out_hbm.at[cut], sems.at[4 + i]))
        copies[-1].start()
    for copy in copies:
        copy.wait()


def plane_kernel(
    in_ref, pot_hbm, *refs
):
    rows = ROWS
    tabs, (out_ref, oh_scr, xl_scr, lo_scr, hi_scr, pot_scr) = refs[:6], refs[6:12]
    copies = fetch(refs[18], *zip(tabs, refs[12:18]), (pot_hbm, pot_scr))
    yf, xe, xo, ie, io, yi = refs[12:18]
    halves = (lo_scr, hi_scr)

    def spot(k, u):
        return (k + u) % 2 * (N // 2) + k * (OWN // 2) + u // 2

    def scatter(i, carry):
        block = in_ref[pl.ds(pl.multiple_of(i * GRP * MSG, 16), GRP * MSG), :].astype(F32)
        for u in range(GRP):
            d = i * GRP + u
            m = block[MSG * u : MSG * (u + 1)]
            xl, y = m[0:1], m[1:2].astype(jnp.int32)
            xl_scr[pl.ds(d, 1), :] = xl
            hot = jnp.where(iota((N, STK), 0) == y, 1.0, 0.0).astype(BF)
            hot = jnp.concatenate([hot, hot[STK:]], axis=0)
            oh_scr[d] = hot
            lhs = jnp.concatenate([jnp.where(xl == k, m[EXT:], 0.0) for k in range(DEP)], axis=0).astype(BF)
            res = dot(lhs, hot, NT)
            for k in range(DEP):
                for r in range(DEP):
                    base = k * rows + r * 8
                    for h in range(2):
                        at = pl.multiple_of((r * N + spot(k, u) + i * (GRP // 2)) * 8, 8)
                        halves[h][pl.ds(at, 8), :] = res[
                            base : base + 8, h * STK : (h + 1) * STK
                        ]
        return carry

    lax.fori_loop(0, OWN // GRP, scatter, 0)
    for copy in copies:
        copy.wait()

    left = iota((N, STK), 1) < STK // 2

    def mixed(one, two):
        return (
            jnp.where(left, one, pltpu.roll(two, STK // 2, 1)),
            jnp.where(left, pltpu.roll(one, STK // 2, 1), two),
        )

    def plane(r, carry):
        at = r * 8 * N
        lined = []
        for b in range(4):
            low = [lo_scr[pl.ds(at + 2 * b + p, N, stride=8), :] for p in range(2)]
            high = [hi_scr[pl.ds(at + 2 * b + p, N, stride=8), :] for p in range(2)]
            lined.append(jnp.concatenate([*low, jnp.where(left, *high)], axis=1).astype(BF))
        ay = jnp.concatenate([dot(jnp.concatenate(lined[c : c + 2], axis=0), yf[...]) for c in (0, 2)], axis=0)
        ay = ay.reshape(4, N, 2 * N)
        blocks = [jnp.concatenate([ay[b, :, :STK], ay[b, :, STK : 2 * STK]], axis=0) for b in range(4)]
        for b in range(0, 4, 2):
            blocks.append(jnp.concatenate(mixed(ay[b, :, 2 * STK :], ay[b + 1, :, 2 * STK :]), axis=0))
        rows = jnp.concatenate(blocks, axis=1).astype(BF)
        fold = N // 2
        one = dot(xe[...], jnp.concatenate([rows[:fold], rows[N : N + fold]], axis=0))
        two = dot(xo[...], jnp.concatenate([rows[fold:N], rows[N + fold :]], axis=0))
        pot = pot_scr[r]
        pot = jnp.concatenate([pot[:, :STK]] * 4 + [pot[:, STK:]] * 4, axis=1)
        near = jnp.concatenate([pot[:fold]] * 2, axis=0)
        far = jnp.concatenate([pot[fold:]] * 2, axis=0)
        near, far = (one + two) * near, (one - two) * far
        one = dot(ie[...], (near + far).astype(BF))
        two = dot(io[...], (near - far).astype(BF))
        bx = jnp.concatenate([one[:fold], two[:fold], one[fold:], two[fold:]], axis=0)
        tails = []
        for b in range(0, 4, 2):
            cut = slice((4 + b // 2) * STK, (5 + b // 2) * STK)
            tails += mixed(bx[:N, cut], bx[N:, cut])
        lined = [
            jnp.concatenate([bx[:N, b * STK : (b + 1) * STK], bx[N:, b * STK : (b + 1) * STK], tails[b]], axis=1)
            for b in range(4)
        ]
        for c in range(0, 4, 2):
            by = dot(jnp.concatenate(lined[c : c + 2], axis=0).astype(BF), yi[...])
            for b in range(2):
                part = by[b * N : (b + 1) * N]
                high = part[:, 2 * STK :]
                for p in range(2):
                    place = pl.ds(at + 2 * (b + c) + p, N, stride=8)
                    lo_scr[place, :] = part[:, p * STK : (p + 1) * STK]
                    hi_scr[place, :] = jnp.where(left, *((high, 0.0) if p == 0 else (0.0, high)))
        return carry

    lax.fori_loop(0, DEP, plane, 0)

    def gather(i, carry):
        parts = []
        for u in range(GRP // 2):
            pair = [2 * u, 2 * u + 1]
            blocks = []
            for d in pair:
                for k in range(DEP):
                    for r in range(DEP):
                        blocks.append(
                            jnp.concatenate(
                                [
                                    half[pl.ds(pl.multiple_of((r * N + spot(k, d) + i * (GRP // 2)) * 8, 8), 8), :]
                                    for half in halves
                                ],
                                axis=1,
                            )
                        )
            lhs = jnp.concatenate(blocks, axis=0).astype(BF)
            res = dot(lhs, jnp.concatenate([oh_scr[i * GRP + d] for d in pair], axis=1))
            for t, d in enumerate(pair):
                xl = xl_scr[pl.ds(i * GRP + d, 1), :]
                took = [
                    res[(t * DEP + k) * rows : (t * DEP + k + 1) * rows, t * STK : (t + 1) * STK] for k in range(DEP)
                ]
                field = jnp.where(xl == 0.0, took[0], jnp.where(xl == 1.0, took[1], took[2]))
                parts += [jnp.zeros((EXT, STK), F32), field]
        out_ref[pl.ds(pl.multiple_of(i * GRP * MSG, 16), GRP * MSG), :] = jnp.concatenate(parts, axis=0).astype(BF)
        return carry

    lax.fori_loop(0, OWN // GRP, gather, 0)


def ready_kernel(
    orb_hbm, slot_hbm, col_hbm, zi_hbm, hot_ref, base_ref, slot_ref, zi_ref, orb_ref, col_ref, sems
):
    copies = fetch(sems, (slot_hbm, slot_ref), (orb_hbm, orb_ref), (col_hbm, col_ref), (zi_hbm, zi_ref))
    for copy in copies:
        copy.wait()
    x, y = column_coords(col_ref[...])
    x = jnp.where(x >= N // 2, x - N, x)
    y = jnp.where(y >= N // 2, y - N, y)
    square = x * x + y * y
    square = jnp.sum(jnp.where(iota((STK, STK), 0) == iota((STK, STK), 1), square, 0.0), axis=1, keepdims=True)

    def step(i, carry):
        cut = pl.ds(pl.multiple_of(i * CUT, CUT), CUT)
        slot = slot_ref[:, cut]
        z, stick = slot >> 7, slot & (STK - 1)
        hot_ref[:, cut] = jnp.where(iota((W, CUT), 0) == (slot & (W - 1)), 1.0, 0.0).astype(BF)
        fz = jnp.where(z >= N // 2, z - N, z).astype(F32)
        flat = jnp.sum(jnp.where(iota((STK, CUT), 0) == stick, square, 0.0), axis=0, keepdims=True)
        kinetic = (fz * fz + flat) * (2.0 / (N * N))
        for b in range(4):
            base_ref[b, :, cut] = kinetic * orb_ref[b, :, cut].astype(F32)
        return carry

    lax.fori_loop(0, hot_ref.shape[1] // CUT, step, 0)


def wave_kernel(in_ref, hot_ref, base_ref, slot_ref, zi_ref, out_ref, sum_ref, m_scr):
    npw = slot_ref.shape[1]

    def unpour(i, total):
        block = in_ref[pl.ds(pl.multiple_of(i * GRP * MSG, 16), GRP * MSG), :].astype(F32)
        for u in range(GRP):
            total = total + block[MSG * u : MSG * u + 1]
            for r in range(DEP):
                row = MSG * u + EXT + 8 * r
                m_scr[r, pl.ds(pl.multiple_of((i * GRP + u) * 8, 8), 8), :] = block[row : row + 8]
        return total

    total = lax.fori_loop(0, OWN // GRP, unpour, jnp.zeros((1, STK), F32))
    total = total[:, 0:8] + total[:, 8:16] + total[:, 16:24]
    sum_ref[...] = jnp.concatenate([total[:, 0:4], total[:, 4:8]], axis=0)
    cols = []
    for b in range(4):
        picks = [m_scr[r, pl.ds(2 * b + p, OWN, stride=8), :] for p in range(2) for r in range(DEP)]
        cols.append(jnp.concatenate(picks, axis=0))
    spectrum = jnp.concatenate(cols, axis=1).astype(BF)
    sticks = dot(zi_ref[...], spectrum).astype(BF)
    fold = N // 2
    sticks = [
        jnp.concatenate(
            [
                jnp.concatenate(
                    [sticks[p * N + q * fold : p * N + (q + 1) * fold, b * STK : (b + 1) * STK] for q in range(2)], axis=1
                )
                for b in range(4)
            ],
            axis=0,
        )
        for p in range(2)
    ]

    def pick(i, carry):
        cut = pl.ds(pl.multiple_of(i * CUT, CUT), CUT)
        hit = iota((fold, CUT), 0) == slot_ref[:, cut] >> 8
        hot = hot_ref[:, cut]
        lines = []
        for p in range(2):
            res = dot(sticks[p], hot)
            lines.append(
                [jnp.sum(jnp.where(hit, res[b * fold : (b + 1) * fold], 0.0), axis=0, keepdims=True) for b in range(4)]
            )
        for b in range(4):
            done = jnp.concatenate([lines[0][b], lines[1][b]], axis=0) + base_ref[b, :, cut]
            out_ref[b, :, cut] = done.astype(BF)
        return carry

    lax.fori_loop(0, npw // CUT, pick, 0, unroll=2)


def overlap_kernel(sub_ref, *refs):
    refs, out_refs = refs[:4], refs[4:]
    sub = sub_ref[...].astype(F32)
    sub = jnp.concatenate([sub[:, 0], sub[:, 1]], axis=1).astype(BF)
    rows = []
    for ref in refs:
        prev = ref[...].astype(F32)
        re, im = prev[:, 0], prev[:, 1]
        rows.append(jnp.concatenate([re, im], axis=1))
        rows.append(jnp.concatenate([im, -re], axis=1))
    res = dot(sub, jnp.concatenate(rows, axis=0).astype(BF), NT)
    top = res.astype(BF).astype(F32)
    mid = (res - top).astype(BF).astype(F32)
    low = res - top - mid
    pad = jnp.zeros((16, STK - 24), F32)
    for k in range(4):
        cut = slice(8 * k, 8 * (k + 1))
        out_refs[k][...] = jnp.concatenate([top[:, cut], mid[:, cut], low[:, cut], pad], axis=1).astype(BF)


def run(kernel, outs, scratch, args, near, room, to=None):
    space = [pltpu.VMEM if n else pltpu.HBM for n in near]
    return pl.pallas_call(
        kernel,
        out_shape=outs,
        in_specs=[pl.BlockSpec(memory_space=m) for m in space],
        **({} if to is None else {"out_specs": pl.BlockSpec(memory_space=to)}),
        scratch_shapes=scratch,
        compiler_params=pltpu.CompilerParams(vmem_limit_bytes=room << 20),
    )(*[pltpu.with_memory_space_constraint(a, m) for a, m in zip(args, space)])


def like(a):
    return pltpu.VMEM(a.shape, a.dtype)


def stage_pack(*args):
    args = (*args, jnp.asarray(tables()["zf"]))
    npw = args[1].shape[1]
    return run(
        pack_kernel,
        pltpu.HBM((OWN * MSG, STK), BF),
        [
            pltpu.VMEM((DEP * STK, npw), BF),
            pltpu.VMEM((512, npw), BF),
            pltpu.VMEM((DEP, OWN * 8, STK), F32),
            pltpu.VMEM((OWN * MSG, STK), BF),
            *map(like, args),
            pltpu.SemaphoreType.DMA((4 + OWN // GRP,)),
        ],
        args,
        (0, 0, 0, 0),
        24,
        pltpu.HBM,
    )


def stage_over(sub, prevs):
    return run(overlap_kernel, [pltpu.VMEM((16, STK), BF)] * 4, [], (sub, *prevs), (1, 1, 1, 1, 1), 8)


def stage_plane(got, pot):
    args = [jnp.asarray(tables()[k]) for k in ("yf", "xe", "xo", "ie", "io", "yi")]
    return run(
        plane_kernel,
        pltpu.VMEM((OWN * MSG, STK), BF),
        [
            pltpu.VMEM((OWN, W, STK), BF),
            pltpu.VMEM((OWN, STK), F32),
            pltpu.VMEM((ROWS * N, STK), F32),
            pltpu.VMEM((ROWS * N, STK), F32),
            like(pot),
            *map(like, args),
            pltpu.SemaphoreType.DMA((7,)),
        ],
        (got, pot, *args),
        (1, 0, 0, 0, 0, 0, 0, 0),
        32,
    )


def stage_ready(orb, slot, col):
    args = (orb, slot, col, jnp.asarray(tables()["zi"]))
    return run(
        ready_kernel,
        [pltpu.VMEM((W, slot.shape[1]), BF), pltpu.VMEM(orb.shape, F32), like(slot), like(args[3])],
        [like(orb), like(col), pltpu.SemaphoreType.DMA((4,))],
        args,
        (0, 0, 0, 0),
        12,
    )


def stage_wave(got, hot, base, slot, zi):
    return run(
        wave_kernel,
        (jax.ShapeDtypeStruct(base.shape, BF), jax.ShapeDtypeStruct((2, 4), F32)),
        [pltpu.VMEM((DEP, OWN * 8, STK), F32)],
        (got, hot, base, slot, zi),
        (1, 1, 1, 1, 1),
        16,
    )


def exchange(tiles):
    return lax.all_to_all(tiles, "fft", 0, 0, tiled=True).reshape(OWN * MSG, STK)


TILES = (OWN, MSG // 2, 2, STK)


def per_device(orbitals, sphere_slot, stick_column, potential, subspace, previous):
    npw = sphere_slot.shape[0]
    slot = sphere_slot.reshape(1, npw)
    col = stick_column.reshape(1, STK)

    def swapped(a, k):
        return lax.ppermute(a, "band", [(g, g ^ k) for g in range(4)])

    across = swapped(previous, 2)
    send = stage_pack(orbitals, slot, col)
    got = exchange(send.reshape(TILES))
    others = [swapped(previous, 1), across, swapped(across, 1)]
    over = stage_over(subspace, [previous, *others])
    mine = [over[0]] + [swapped(over[k], k) for k in (1, 2, 3)]
    prepared = stage_ready(orbitals, slot, col)
    field = stage_plane(got, potential)
    group = lax.axis_index("band")
    for k in (1, 2):
        mine = [jnp.where((group & k) > 0, mine[i ^ k], mine[i]) for i in range(4)]
    sums = jnp.concatenate(mine, axis=0).reshape(OWN, 1, 1, STK)
    head = jnp.pad(sums, ((0, 0), (0, 0), (0, EXT - 1), (0, 0)))
    back = exchange(lax.dynamic_update_slice(field.reshape(TILES), head, (0, 0, 0, 0)))
    applied, total = stage_wave(back, *prepared)
    return applied, total.reshape(2, 1, 4)


def solution(mesh):
    return jax.shard_map(
        per_device,
        mesh=mesh,
        in_specs=(
            P("band", None, "fft"),
            P("fft"),
            P("fft"),
            P("fft", None, None),
            P("band", None, "fft"),
            P("band", None, "fft"),
        ),
        out_specs=(P("band", None, "fft"), P(None, "fft", "band")),
        check_vma=False,
    )
```

```python
import functools
import math

import jax
import jax.numpy as jnp
import numpy as np
from jax import lax
from jax.experimental import pallas as pl
from jax.experimental.pallas import tpu as pltpu
from jax.sharding import PartitionSpec as P


BF = jnp.bfloat16
F32 = jnp.float32
N = 192
OWN = 64
DEP = N // OWN
STK = 128
W = 256
ROWS = 8 * DEP
EXT = 2
MSG = EXT + ROWS
GRP = 16
CUT = 512
NT = (((1,), (1,)), ((), ()))


def dot(a, b, dims=(((1,), (0,)), ((), ()))):
    return lax.dot_general(a, b, dims, preferred_element_type=F32)


@functools.cache
def tables():
    def trig(rows, cols, scale):
        angle = (np.outer(rows, cols) % N) * (2.0 * math.pi / N)
        return np.cos(angle) * scale, np.sin(angle) * scale

    nat = np.arange(N)
    dealt = (np.arange(DEP)[:, None] + DEP * np.arange(OWN)[None, :]).reshape(-1)

    half = nat[: N // 2]
    even, odd = (
        np.concatenate([part + DEP * (2 * np.arange(OWN // 2) + (part + q) % 2) for part in range(DEP)]) for q in range(2)
    )
    assert not (even % 2).any() and (odd % 2).all()

    def wide(a, rows, cols):
        out = np.zeros((rows, cols))
        out[: a.shape[0], : a.shape[1]] = a
        return out

    def left(rows, cols, scale, sign, width):
        c, s = trig(rows, cols, scale)
        c, s = wide(c, len(rows), width), wide(s * sign, len(rows), width)
        return np.block([[c, -s], [s, c]])

    def right(rows, cols, scale, sign, order, width):
        c, s = trig(rows, cols, scale)
        c, s = wide(c, N, width), wide(s * sign, N, width)
        full = np.block([[c, s], [-s, c]])
        return full if order is None else full[np.ix_(order, order)]

    packed = np.concatenate([np.arange(128), N + np.arange(128), np.arange(128, N), np.arange(N + 128, 2 * N)])
    by_block = np.arange(2 * N).reshape(2, DEP, 64).transpose(1, 0, 2).reshape(-1)
    inv = 1.0 / N
    out = {
        "zf": left(dealt, nat, 1.0, 1.0, N)[:, by_block],
        "yf": right(nat, nat, 1.0, 1.0, packed, N),
        "xe": left(half, even, 1.0, 1.0, N // 2),
        "xo": left(half, odd, 1.0, 1.0, N // 2),
        "ie": left(even, half, inv, -1.0, N // 2),
        "io": left(odd, half, inv, -1.0, N // 2),
        "yi": right(nat, nat, inv, -1.0, packed, N),
        "zi": left(np.concatenate([nat[::2], nat[1::2]]), dealt, inv, -1.0, N),
    }
    return {k: v.astype(np.float32).astype(BF) for k, v in out.items()}


def iota(shape, dim):
    return lax.broadcasted_iota(jnp.int32, shape, dim)


def column_coords(col):
    c = col.astype(F32)
    x = jnp.floor((c + 0.5) * (1.0 / N))
    return x, c - x * N


def fetch(sems, *pairs):
    copies = [pltpu.make_async_copy(src, dst, sems.at[i]) for i, (src, dst) in enumerate(pairs)]
    for copy in copies:
        copy.start()
    return copies


def pack_kernel(
    orb_hbm, slot_hbm, col_hbm, zf_hbm, out_hbm, a_scr, b_scr, m_scr, out_ref, orb_ref, slot_ref, col_ref, zf_ref, sems
):
    copies = fetch(sems, (slot_hbm, slot_ref), (orb_hbm, orb_ref), (col_hbm, col_ref), (zf_hbm, zf_ref))
    npw = slot_ref.shape[1]
    copies[0].wait()
    slot = slot_ref[...]
    low = (slot >> 7) & 63
    high = (slot >> 13) * STK + (slot & (STK - 1))
    half = 1024
    copies[1].wait()
    for i in range(0, npw, half):
        cut = slice(i, i + half)
        a_scr[:, cut] = jnp.where(iota((DEP * STK, half), 0) == high[:, cut], 1.0, 0.0).astype(BF)
        hit = iota((64, half), 0) == low[:, cut]
        for j in range(8):
            row = orb_ref[j // 2, j % 2 : j % 2 + 1, cut].astype(F32)
            b_scr[64 * j : 64 * (j + 1), cut] = jnp.where(hit, row, 0.0).astype(BF)
    grid = dot(a_scr[...], b_scr[...], NT).astype(BF)
    stick = jnp.concatenate(
        [
            jnp.concatenate([grid[STK * h : STK * (h + 1), STK * b : STK * (b + 1)] for h in range(DEP)], axis=1)
            for b in range(4)
        ],
        axis=0,
    )
    copies[2].wait()
    copies[3].wait()
    wave = dot(zf_ref[...], stick, NT)
    x, y = column_coords(col_ref[...])
    xl = x - DEP * jnp.floor((x + 0.5) * (1.0 / DEP))
    ext = jnp.concatenate([xl, y], axis=0)
    for r in range(DEP):
        for j in range(8):
            base = (j % 2) * N + r * OWN
            m_scr[r, pl.ds(j, OWN, stride=8), :] = wave[base : base + OWN, STK * (j // 2) : STK * (j // 2 + 1)]

    copies = []
    for i in range(OWN // GRP):
        parts = []
        for u in range(i * GRP, (i + 1) * GRP):
            parts += [ext] + [m_scr[r, 8 * u : 8 * u + 8] for r in range(DEP)]
        cut = pl.ds(i * GRP * MSG, GRP * MSG)
        out_ref[cut, :] = jnp.concatenate(parts, axis=0).astype(BF)
        copies.append(pltpu.make_async_copy(out_ref.at[cut], out_hbm.at[cut], sems.at[4 + i]))
        copies[-1].start()
    for copy in copies:
        copy.wait()


def plane_kernel(
    in_ref, pot_hbm, *refs
):
    rows = ROWS
    tabs, (out_ref, oh_scr, xl_scr, lo_scr, hi_scr, pot_scr) = refs[:6], refs[6:12]
    copies = fetch(refs[18], *zip(tabs, refs[12:18]), (pot_hbm, pot_scr))
    yf, xe, xo, ie, io, yi = refs[12:18]
    halves = (lo_scr, hi_scr)

    def spot(k, u):
        return (k + u) % 2 * (N // 2) + k * (OWN // 2) + u // 2

    rise = iota((N, STK), 0).astype(F32).astype(BF)

    def scatter(i, carry):
        block = in_ref[pl.ds(pl.multiple_of(i * GRP * MSG, 16), GRP * MSG), :].astype(F32)
        for u in range(GRP):
            d = i * GRP + u
            m = block[MSG * u : MSG * (u + 1)]
            xl, y = m[0:1], m[1:2].astype(BF)
            xl_scr[pl.ds(d, 1), :] = xl
            hot = jnp.where(rise == y, BF(1), BF(0))
            hot = jnp.concatenate([hot, hot[STK:]], axis=0)
            oh_scr[d] = hot
            lhs = jnp.concatenate([jnp.where(xl == k, m[EXT:], 0.0) for k in range(DEP)], axis=0).astype(BF)
            res = dot(lhs, hot, NT)
            for k in range(DEP):
                for r in range(DEP):
                    base = k * rows + r * 8
                    for h in range(2):
                        at = pl.multiple_of((r * N + spot(k, u) + i * (GRP // 2)) * 8, 8)
                        halves[h][pl.ds(at, 8), :] = res[
                            base : base + 8, h * STK : (h + 1) * STK
                        ]
        return carry

    lax.fori_loop(0, OWN // GRP, scatter, 0)
    for copy in copies:
        copy.wait()

    left = iota((N, STK), 1) < STK // 2

    def mixed(one, two):
        return (
            jnp.where(left, one, pltpu.roll(two, STK // 2, 1)),
            jnp.where(left, pltpu.roll(one, STK // 2, 1), two),
        )

    def plane(r, carry):
        at = r * 8 * N
        lined = []
        for b in range(4):
            low = [lo_scr[pl.ds(at + 2 * b + p, N, stride=8), :] for p in range(2)]
            high = [hi_scr[pl.ds(at + 2 * b + p, N, stride=8), :] for p in range(2)]
            lined.append(jnp.concatenate([*low, jnp.where(left, *high)], axis=1).astype(BF))
        ay = jnp.concatenate([dot(jnp.concatenate(lined[c : c + 2], axis=0), yf[...]) for c in (0, 2)], axis=0)
        ay = ay.reshape(4, N, 2 * N)
        blocks = [jnp.concatenate([ay[b, :, :STK], ay[b, :, STK : 2 * STK]], axis=0) for b in range(4)]
        for b in range(0, 4, 2):
            blocks.append(jnp.concatenate(mixed(ay[b, :, 2 * STK :], ay[b + 1, :, 2 * STK :]), axis=0))
        rows = jnp.concatenate(blocks, axis=1).astype(BF)
        fold = N // 2
        one = dot(xe[...], jnp.concatenate([rows[:fold], rows[N : N + fold]], axis=0))
        two = dot(xo[...], jnp.concatenate([rows[fold:N], rows[N + fold :]], axis=0))
        pot = pot_scr[r]
        pot = jnp.concatenate([pot[:, :STK]] * 4 + [pot[:, STK:]] * 4, axis=1)
        near = jnp.concatenate([pot[:fold]] * 2, axis=0)
        far = jnp.concatenate([pot[fold:]] * 2, axis=0)
        near, far = (one + two) * near, (one - two) * far
        one = dot(ie[...], (near + far).astype(BF))
        two = dot(io[...], (near - far).astype(BF))
        bx = jnp.concatenate([one[:fold], two[:fold], one[fold:], two[fold:]], axis=0)
        tails = []
        for b in range(0, 4, 2):
            cut = slice((4 + b // 2) * STK, (5 + b // 2) * STK)
            tails += mixed(bx[:N, cut], bx[N:, cut])
        lined = [
            jnp.concatenate([bx[:N, b * STK : (b + 1) * STK], bx[N:, b * STK : (b + 1) * STK], tails[b]], axis=1)
            for b in range(4)
        ]
        for c in range(0, 4, 2):
            by = dot(jnp.concatenate(lined[c : c + 2], axis=0).astype(BF), yi[...])
            for b in range(2):
                part = by[b * N : (b + 1) * N]
                high = part[:, 2 * STK :]
                for p in range(2):
                    place = pl.ds(at + 2 * (b + c) + p, N, stride=8)
                    lo_scr[place, :] = part[:, p * STK : (p + 1) * STK]
                    hi_scr[place, :] = jnp.where(left, *((high, 0.0) if p == 0 else (0.0, high)))
        return carry

    lax.fori_loop(0, DEP, plane, 0)

    def gather(i, carry):
        parts = []
        for u in range(GRP // 2):
            pair = [2 * u, 2 * u + 1]
            blocks = []
            for d in pair:
                for k in range(DEP):
                    for r in range(DEP):
                        blocks.append(
                            jnp.concatenate(
                                [
                                    half[pl.ds(pl.multiple_of((r * N + spot(k, d) + i * (GRP // 2)) * 8, 8), 8), :]
                                    for half in halves
                                ],
                                axis=1,
                            )
                        )
            lhs = jnp.concatenate(blocks, axis=0).astype(BF)
            res = dot(lhs, jnp.concatenate([oh_scr[i * GRP + d] for d in pair], axis=1))
            for t, d in enumerate(pair):
                xl = xl_scr[pl.ds(i * GRP + d, 1), :]
                took = [
                    res[(t * DEP + k) * rows : (t * DEP + k + 1) * rows, t * STK : (t + 1) * STK] for k in range(DEP)
                ]
                field = jnp.where(xl == 0.0, took[0], jnp.where(xl == 1.0, took[1], took[2]))
                parts += [jnp.zeros((EXT, STK), F32), field]
        out_ref[pl.ds(pl.multiple_of(i * GRP * MSG, 16), GRP * MSG), :] = jnp.concatenate(parts, axis=0).astype(BF)
        return carry

    lax.fori_loop(0, OWN // GRP, gather, 0)


def ready_kernel(
    orb_hbm, slot_hbm, col_hbm, zi_hbm, hot_ref, base_ref, slot_ref, zi_ref, orb_ref, col_ref, sems
):
    copies = fetch(sems, (slot_hbm, slot_ref), (orb_hbm, orb_ref), (col_hbm, col_ref), (zi_hbm, zi_ref))
    for copy in copies:
        copy.wait()
    x, y = column_coords(col_ref[...])
    x = jnp.where(x >= N // 2, x - N, x)
    y = jnp.where(y >= N // 2, y - N, y)
    square = x * x + y * y
    square = jnp.sum(jnp.where(iota((STK, STK), 0) == iota((STK, STK), 1), square, 0.0), axis=1, keepdims=True)

    def step(i, carry):
        cut = pl.ds(pl.multiple_of(i * CUT, CUT), CUT)
        slot = slot_ref[:, cut]
        z, stick = slot >> 7, slot & (STK - 1)
        hot_ref[:, cut] = jnp.where(iota((W, CUT), 0) == (slot & (W - 1)), 1.0, 0.0).astype(BF)
        fz = jnp.where(z >= N // 2, z - N, z).astype(F32)
        flat = jnp.sum(jnp.where(iota((STK, CUT), 0) == stick, square, 0.0), axis=0, keepdims=True)
        kinetic = (fz * fz + flat) * (2.0 / (N * N))
        for b in range(4):
            base_ref[b, :, cut] = kinetic * orb_ref[b, :, cut].astype(F32)
        return carry

    lax.fori_loop(0, hot_ref.shape[1] // CUT, step, 0)


def wave_kernel(in_ref, hot_ref, base_ref, slot_ref, zi_ref, out_ref, sum_ref, m_scr):
    npw = slot_ref.shape[1]

    def unpour(i, total):
        block = in_ref[pl.ds(pl.multiple_of(i * GRP * MSG, 16), GRP * MSG), :].astype(F32)
        for u in range(GRP):
            total = total + block[MSG * u : MSG * u + 1]
            for r in range(DEP):
                row = MSG * u + EXT + 8 * r
                m_scr[r, pl.ds(pl.multiple_of((i * GRP + u) * 8, 8), 8), :] = block[row : row + 8]
        return total

    total = lax.fori_loop(0, OWN // GRP, unpour, jnp.zeros((1, STK), F32))
    total = total[:, 0:8] + total[:, 8:16] + total[:, 16:24]
    sum_ref[...] = jnp.concatenate([total[:, 0:4], total[:, 4:8]], axis=0)
    cols = []
    for b in range(4):
        picks = [m_scr[r, pl.ds(2 * b + p, OWN, stride=8), :] for p in range(2) for r in range(DEP)]
        cols.append(jnp.concatenate(picks, axis=0))
    spectrum = jnp.concatenate(cols, axis=1).astype(BF)
    sticks = dot(zi_ref[...], spectrum).astype(BF)
    fold = N // 2
    sticks = [
        jnp.concatenate(
            [
                jnp.concatenate(
                    [sticks[p * N + q * fold : p * N + (q + 1) * fold, b * STK : (b + 1) * STK] for q in range(2)], axis=1
                )
                for b in range(4)
            ],
            axis=0,
        )
        for p in range(2)
    ]

    def pick(i, carry):
        cut = pl.ds(pl.multiple_of(i * CUT, CUT), CUT)
        hit = iota((fold, CUT), 0) == slot_ref[:, cut] >> 8
        hot = hot_ref[:, cut]
        lines = []
        for p in range(2):
            res = dot(sticks[p], hot)
            lines.append(
                [jnp.sum(jnp.where(hit, res[b * fold : (b + 1) * fold], 0.0), axis=0, keepdims=True) for b in range(4)]
            )
        for b in range(4):
            done = jnp.concatenate([lines[0][b], lines[1][b]], axis=0) + base_ref[b, :, cut]
            out_ref[b, :, cut] = done.astype(BF)
        return carry

    lax.fori_loop(0, npw // CUT, pick, 0, unroll=4)


def overlap_kernel(sub_ref, *refs):
    refs, out_refs = refs[:4], refs[4:]
    sub = sub_ref[...].astype(F32)
    sub = jnp.concatenate([sub[:, 0], sub[:, 1]], axis=1).astype(BF)
    rows = []
    for ref in refs:
        prev = ref[...].astype(F32)
        re, im = prev[:, 0], prev[:, 1]
        rows.append(jnp.concatenate([re, im], axis=1))
        rows.append(jnp.concatenate([im, -re], axis=1))
    res = dot(sub, jnp.concatenate(rows, axis=0).astype(BF), NT)
    top = res.astype(BF).astype(F32)
    mid = (res - top).astype(BF).astype(F32)
    low = res - top - mid
    pad = jnp.zeros((16, STK - 24), F32)
    for k in range(4):
        cut = slice(8 * k, 8 * (k + 1))
        out_refs[k][...] = jnp.concatenate([top[:, cut], mid[:, cut], low[:, cut], pad], axis=1).astype(BF)


def run(kernel, outs, scratch, args, near, room, to=None):
    space = [pltpu.VMEM if n else pltpu.HBM for n in near]
    return pl.pallas_call(
        kernel,
        out_shape=outs,
        in_specs=[pl.BlockSpec(memory_space=m) for m in space],
        **({} if to is None else {"out_specs": pl.BlockSpec(memory_space=to)}),
        scratch_shapes=scratch,
        compiler_params=pltpu.CompilerParams(vmem_limit_bytes=room << 20),
    )(*[pltpu.with_memory_space_constraint(a, m) for a, m in zip(args, space)])


def like(a):
    return pltpu.VMEM(a.shape, a.dtype)


def stage_pack(*args):
    args = (*args, jnp.asarray(tables()["zf"]))
    npw = args[1].shape[1]
    return run(
        pack_kernel,
        pltpu.HBM((OWN * MSG, STK), BF),
        [
            pltpu.VMEM((DEP * STK, npw), BF),
            pltpu.VMEM((512, npw), BF),
            pltpu.VMEM((DEP, OWN * 8, STK), F32),
            pltpu.VMEM((OWN * MSG, STK), BF),
            *map(like, args),
            pltpu.SemaphoreType.DMA((4 + OWN // GRP,)),
        ],
        args,
        (0, 0, 0, 0),
        24,
        pltpu.HBM,
    )


def stage_over(sub, prevs):
    return run(overlap_kernel, [pltpu.VMEM((16, STK), BF)] * 4, [], (sub, *prevs), (1, 1, 1, 1, 1), 8)


def stage_plane(got, pot):
    args = [jnp.asarray(tables()[k]) for k in ("yf", "xe", "xo", "ie", "io", "yi")]
    return run(
        plane_kernel,
        pltpu.VMEM((OWN * MSG, STK), BF),
        [
            pltpu.VMEM((OWN, W, STK), BF),
            pltpu.VMEM((OWN, STK), F32),
            pltpu.VMEM((ROWS * N, STK), F32),
            pltpu.VMEM((ROWS * N, STK), F32),
            like(pot),
            *map(like, args),
            pltpu.SemaphoreType.DMA((7,)),
        ],
        (got, pot, *args),
        (1, 0, 0, 0, 0, 0, 0, 0),
        32,
    )


def stage_ready(orb, slot, col):
    args = (orb, slot, col, jnp.asarray(tables()["zi"]))
    return run(
        ready_kernel,
        [pltpu.VMEM((W, slot.shape[1]), BF), pltpu.VMEM(orb.shape, F32), like(slot), like(args[3])],
        [like(orb), like(col), pltpu.SemaphoreType.DMA((4,))],
        args,
        (0, 0, 0, 0),
        12,
    )


def stage_wave(got, hot, base, slot, zi):
    return run(
        wave_kernel,
        (jax.ShapeDtypeStruct(base.shape, BF), jax.ShapeDtypeStruct((2, 4), F32)),
        [pltpu.VMEM((DEP, OWN * 8, STK), F32)],
        (got, hot, base, slot, zi),
        (1, 1, 1, 1, 1),
        16,
    )


def exchange(tiles):
    return lax.all_to_all(tiles, "fft", 0, 0, tiled=True).reshape(OWN * MSG, STK)


TILES = (OWN, MSG // 2, 2, STK)


def per_device(orbitals, sphere_slot, stick_column, potential, subspace, previous):
    npw = sphere_slot.shape[0]
    slot = sphere_slot.reshape(1, npw)
    col = stick_column.reshape(1, STK)

    def swapped(a, k):
        return lax.ppermute(a, "band", [(g, g ^ k) for g in range(4)])

    across = swapped(previous, 2)
    send = stage_pack(orbitals, slot, col)
    got = exchange(send.reshape(TILES))
    others = [swapped(previous, 1), across, swapped(across, 1)]
    over = stage_over(subspace, [previous, *others])
    mine = [over[0]] + [swapped(over[k], k) for k in (1, 2, 3)]
    prepared = stage_ready(orbitals, slot, col)
    field = stage_plane(got, potential)
    group = lax.axis_index("band")
    for k in (1, 2):
        mine = [jnp.where((group & k) > 0, mine[i ^ k], mine[i]) for i in range(4)]
    sums = jnp.concatenate(mine, axis=0).reshape(OWN, 1, 1, STK)
    head = jnp.pad(sums, ((0, 0), (0, 0), (0, EXT - 1), (0, 0)))
    back = exchange(lax.dynamic_update_slice(field.reshape(TILES), head, (0, 0, 0, 0)))
    applied, total = stage_wave(back, *prepared)
    return applied, total.reshape(2, 1, 4)


def solution(mesh):
    return jax.shard_map(
        per_device,
        mesh=mesh,
        in_specs=(
            P("band", None, "fft"),
            P("fft"),
            P("fft"),
            P("fft", None, None),
            P("band", None, "fft"),
            P("band", None, "fft"),
        ),
        out_specs=(P("band", None, "fft"), P(None, "fft", "band")),
        check_vma=False,
    )
```

```python
import functools
import math

import jax
import jax.numpy as jnp
import numpy as np
from jax import lax
from jax.experimental import pallas as pl
from jax.experimental.pallas import tpu as pltpu
from jax.sharding import PartitionSpec as P


BF = jnp.bfloat16
F32 = jnp.float32
N = 192
OWN = 64
DEP = N // OWN
STK = 128
W = 256
ROWS = 8 * DEP
EXT = 2
MSG = EXT + ROWS
GRP = 16
CUT = 512
NT = (((1,), (1,)), ((), ()))


def dot(a, b, dims=(((1,), (0,)), ((), ()))):
    return lax.dot_general(a, b, dims, preferred_element_type=F32)


@functools.cache
def tables():
    def trig(rows, cols, scale):
        angle = (np.outer(rows, cols) % N) * (2.0 * math.pi / N)
        return np.cos(angle) * scale, np.sin(angle) * scale

    nat = np.arange(N)
    dealt = (np.arange(DEP)[:, None] + DEP * np.arange(OWN)[None, :]).reshape(-1)

    half = nat[: N // 2]
    even, odd = (
        np.concatenate([part + DEP * (2 * np.arange(OWN // 2) + (part + q) % 2) for part in range(DEP)]) for q in range(2)
    )
    assert not (even % 2).any() and (odd % 2).all()

    def wide(a, rows, cols):
        out = np.zeros((rows, cols))
        out[: a.shape[0], : a.shape[1]] = a
        return out

    def left(rows, cols, scale, sign, width):
        c, s = trig(rows, cols, scale)
        c, s = wide(c, len(rows), width), wide(s * sign, len(rows), width)
        return np.block([[c, -s], [s, c]])

    def right(rows, cols, scale, sign, order, width):
        c, s = trig(rows, cols, scale)
        c, s = wide(c, N, width), wide(s * sign, N, width)
        full = np.block([[c, s], [-s, c]])
        return full if order is None else full[np.ix_(order, order)]

    packed = np.concatenate([np.arange(128), N + np.arange(128), np.arange(128, N), np.arange(N + 128, 2 * N)])
    by_block = np.arange(2 * N).reshape(2, DEP, 64).transpose(1, 0, 2).reshape(-1)
    inv = 1.0 / N
    out = {
        "zf": left(dealt, nat, 1.0, 1.0, N)[:, by_block],
        "yf": right(nat, nat, 1.0, 1.0, packed, N),
        "xe": left(half, even, 1.0, 1.0, N // 2),
        "xo": left(half, odd, 1.0, 1.0, N // 2),
        "ie": left(even, half, inv, -1.0, N // 2),
        "io": left(odd, half, inv, -1.0, N // 2),
        "yi": right(nat, nat, inv, -1.0, packed, N),
        "zi": left(np.concatenate([nat[::2], nat[1::2]]), dealt, inv, -1.0, N),
    }
    return {k: v.astype(np.float32).astype(BF) for k, v in out.items()}


def iota(shape, dim):
    return lax.broadcasted_iota(jnp.int32, shape, dim)


def column_coords(col):
    c = col.astype(F32)
    x = jnp.floor((c + 0.5) * (1.0 / N))
    return x, c - x * N


def fetch(sems, *pairs):
    copies = [pltpu.make_async_copy(src, dst, sems.at[i]) for i, (src, dst) in enumerate(pairs)]
    for copy in copies:
        copy.start()
    return copies


def pack_kernel(
    orb_hbm, slot_hbm, col_hbm, zf_hbm, out_hbm, a_scr, b_scr, m_scr, out_ref, orb_ref, slot_ref, col_ref, zf_ref, sems
):
    copies = fetch(sems, (slot_hbm, slot_ref), (orb_hbm, orb_ref), (col_hbm, col_ref), (zf_hbm, zf_ref))
    npw = slot_ref.shape[1]
    copies[0].wait()
    slot = slot_ref[...]
    low = (slot >> 7) & 63
    high = (slot >> 13)
    stick = slot & (STK - 1)
    rise = iota((STK, 1024), 0).astype(F32).astype(BF)
    half = 1024
    copies[1].wait()
    for i in range(0, npw, half):
        cut = slice(i, i + half)
        for h in range(DEP):
            mine = jnp.where(high[:, cut] == h, stick[:, cut], -1).astype(F32).astype(BF)
            a_scr[STK * h : STK * (h + 1), cut] = jnp.where(rise == mine, BF(1), BF(0))
        hit = rise[:64] == low[:, cut].astype(F32).astype(BF)
        for j in range(8):
            row = orb_ref[j // 2, j % 2 : j % 2 + 1, cut]
            b_scr[64 * j : 64 * (j + 1), cut] = jnp.where(hit, row, BF(0))
    grid = dot(a_scr[...], b_scr[...], NT).astype(BF)
    stick = jnp.concatenate(
        [
            jnp.concatenate([grid[STK * h : STK * (h + 1), STK * b : STK * (b + 1)] for h in range(DEP)], axis=1)
            for b in range(4)
        ],
        axis=0,
    )
    copies[2].wait()
    copies[3].wait()
    wave = dot(zf_ref[...], stick, NT)
    x, y = column_coords(col_ref[...])
    xl = x - DEP * jnp.floor((x + 0.5) * (1.0 / DEP))
    ext = jnp.concatenate([xl, y], axis=0)
    for r in range(DEP):
        for j in range(8):
            base = (j % 2) * N + r * OWN
            m_scr[r, pl.ds(j, OWN, stride=8), :] = wave[base : base + OWN, STK * (j // 2) : STK * (j // 2 + 1)]

    copies = []
    for i in range(OWN // GRP):
        parts = []
        for u in range(i * GRP, (i + 1) * GRP):
            parts += [ext] + [m_scr[r, 8 * u : 8 * u + 8] for r in range(DEP)]
        cut = pl.ds(i * GRP * MSG, GRP * MSG)
        out_ref[cut, :] = jnp.concatenate(parts, axis=0).astype(BF)
        copies.append(pltpu.make_async_copy(out_ref.at[cut], out_hbm.at[cut], sems.at[4 + i]))
        copies[-1].start()
    for copy in copies:
        copy.wait()


def plane_kernel(
    in_ref, pot_hbm, *refs
):
    rows = ROWS
    tabs, (out_ref, oh_scr, xl_scr, lo_scr, hi_scr, pot_scr) = refs[:6], refs[6:12]
    copies = fetch(refs[18], *zip(tabs, refs[12:18]), (pot_hbm, pot_scr))
    yf, xe, xo, ie, io, yi = refs[12:18]
    halves = (lo_scr, hi_scr)

    def spot(k, u):
        return (k + u) % 2 * (N // 2) + k * (OWN // 2) + u // 2

    rise = iota((N, STK), 0).astype(F32).astype(BF)

    def scatter(i, carry):
        block = in_ref[pl.ds(pl.multiple_of(i * GRP * MSG, 16), GRP * MSG), :].astype(F32)
        for u in range(GRP):
            d = i * GRP + u
            m = block[MSG * u : MSG * (u + 1)]
            xl, y = m[0:1], m[1:2].astype(BF)
            xl_scr[pl.ds(d, 1), :] = xl
            hot = jnp.where(rise == y, BF(1), BF(0))
            hot = jnp.concatenate([hot, hot[STK:]], axis=0)
            oh_scr[d] = hot
            lhs = jnp.concatenate([jnp.where(xl == k, m[EXT:], 0.0) for k in range(DEP)], axis=0).astype(BF)
            res = dot(lhs, hot, NT)
            for k in range(DEP):
                for r in range(DEP):
                    base = k * rows + r * 8
                    for h in range(2):
                        at = pl.multiple_of((r * N + spot(k, u) + i * (GRP // 2)) * 8, 8)
                        halves[h][pl.ds(at, 8), :] = res[
                            base : base + 8, h * STK : (h + 1) * STK
                        ]
        return carry

    lax.fori_loop(0, OWN // GRP, scatter, 0)
    for copy in copies:
        copy.wait()

    left = iota((N, STK), 1) < STK // 2

    def mixed(one, two):
        return (
            jnp.where(left, one, pltpu.roll(two, STK // 2, 1)),
            jnp.where(left, pltpu.roll(one, STK // 2, 1), two),
        )

    def plane(r, carry):
        at = r * 8 * N
        lined = []
        for b in range(4):
            low = [lo_scr[pl.ds(at + 2 * b + p, N, stride=8), :] for p in range(2)]
            high = [hi_scr[pl.ds(at + 2 * b + p, N, stride=8), :] for p in range(2)]
            lined.append(jnp.concatenate([*low, jnp.where(left, *high)], axis=1).astype(BF))
        ay = jnp.concatenate([dot(jnp.concatenate(lined[c : c + 2], axis=0), yf[...]) for c in (0, 2)], axis=0)
        ay = ay.reshape(4, N, 2 * N)
        blocks = [jnp.concatenate([ay[b, :, :STK], ay[b, :, STK : 2 * STK]], axis=0) for b in range(4)]
        for b in range(0, 4, 2):
            blocks.append(jnp.concatenate(mixed(ay[b, :, 2 * STK :], ay[b + 1, :, 2 * STK :]), axis=0))
        rows = jnp.concatenate(blocks, axis=1).astype(BF)
        fold = N // 2
        one = dot(xe[...], jnp.concatenate([rows[:fold], rows[N : N + fold]], axis=0))
        two = dot(xo[...], jnp.concatenate([rows[fold:N], rows[N + fold :]], axis=0))
        pot = pot_scr[r]
        pot = jnp.concatenate([pot[:, :STK]] * 4 + [pot[:, STK:]] * 4, axis=1)
        near = jnp.concatenate([pot[:fold]] * 2, axis=0)
        far = jnp.concatenate([pot[fold:]] * 2, axis=0)
        near, far = (one + two) * near, (one - two) * far
        one = dot(ie[...], (near + far).astype(BF))
        two = dot(io[...], (near - far).astype(BF))
        bx = jnp.concatenate([one[:fold], two[:fold], one[fold:], two[fold:]], axis=0)
        tails = []
        for b in range(0, 4, 2):
            cut = slice((4 + b // 2) * STK, (5 + b // 2) * STK)
            tails += mixed(bx[:N, cut], bx[N:, cut])
        lined = [
            jnp.concatenate([bx[:N, b * STK : (b + 1) * STK], bx[N:, b * STK : (b + 1) * STK], tails[b]], axis=1)
            for b in range(4)
        ]
        for c in range(0, 4, 2):
            by = dot(jnp.concatenate(lined[c : c + 2], axis=0).astype(BF), yi[...])
            for b in range(2):
                part = by[b * N : (b + 1) * N]
                high = part[:, 2 * STK :]
                for p in range(2):
                    place = pl.ds(at + 2 * (b + c) + p, N, stride=8)
                    lo_scr[place, :] = part[:, p * STK : (p + 1) * STK]
                    hi_scr[place, :] = jnp.where(left, *((high, 0.0) if p == 0 else (0.0, high)))
        return carry

    lax.fori_loop(0, DEP, plane, 0, unroll=True)

    def gather(i, carry):
        parts = []
        for u in range(GRP // 2):
            pair = [2 * u, 2 * u + 1]
            blocks = []
            for d in pair:
                for k in range(DEP):
                    for r in range(DEP):
                        blocks.append(
                            jnp.concatenate(
                                [
                                    half[pl.ds(pl.multiple_of((r * N + spot(k, d) + i * (GRP // 2)) * 8, 8), 8), :]
                                    for half in halves
                                ],
                                axis=1,
                            )
                        )
            lhs = jnp.concatenate(blocks, axis=0).astype(BF)
            res = dot(lhs, jnp.concatenate([oh_scr[i * GRP + d] for d in pair], axis=1))
            for t, d in enumerate(pair):
                xl = xl_scr[pl.ds(i * GRP + d, 1), :]
                took = [
                    res[(t * DEP + k) * rows : (t * DEP + k + 1) * rows, t * STK : (t + 1) * STK] for k in range(DEP)
                ]
                field = jnp.where(xl == 0.0, took[0], jnp.where(xl == 1.0, took[1], took[2]))
                parts += [jnp.zeros((EXT, STK), F32), field]
        out_ref[pl.ds(pl.multiple_of(i * GRP * MSG, 16), GRP * MSG), :] = jnp.concatenate(parts, axis=0).astype(BF)
        return carry

    lax.fori_loop(0, OWN // GRP, gather, 0, unroll=True)


def ready_kernel(
    orb_hbm, slot_hbm, col_hbm, zi_hbm, hot_ref, base_ref, slot_ref, zi_ref, orb_ref, col_ref, sems
):
    copies = fetch(sems, (slot_hbm, slot_ref), (orb_hbm, orb_ref), (col_hbm, col_ref), (zi_hbm, zi_ref))
    for copy in copies:
        copy.wait()
    x, y = column_coords(col_ref[...])
    x = jnp.where(x >= N // 2, x - N, x)
    y = jnp.where(y >= N // 2, y - N, y)
    square = x * x + y * y
    square = jnp.sum(jnp.where(iota((STK, STK), 0) == iota((STK, STK), 1), square, 0.0), axis=1, keepdims=True)

    def step(i, carry):
        cut = pl.ds(pl.multiple_of(i * CUT, CUT), CUT)
        slot = slot_ref[:, cut]
        z, stick = slot >> 7, slot & (STK - 1)
        hot_ref[:, cut] = jnp.where(iota((W, CUT), 0) == (slot & (W - 1)), 1.0, 0.0).astype(BF)
        fz = jnp.where(z >= N // 2, z - N, z).astype(F32)
        flat = jnp.sum(jnp.where(iota((STK, CUT), 0) == stick, square, 0.0), axis=0, keepdims=True)
        kinetic = (fz * fz + flat) * (2.0 / (N * N))
        for b in range(4):
            base_ref[b, :, cut] = kinetic * orb_ref[b, :, cut].astype(F32)
        return carry

    lax.fori_loop(0, hot_ref.shape[1] // CUT, step, 0)


def wave_kernel(in_ref, hot_ref, base_ref, slot_ref, zi_ref, out_ref, sum_ref, m_scr):
    npw = slot_ref.shape[1]

    def unpour(i, total):
        block = in_ref[pl.ds(pl.multiple_of(i * GRP * MSG, 16), GRP * MSG), :].astype(F32)
        for u in range(GRP):
            total = total + block[MSG * u : MSG * u + 1]
            for r in range(DEP):
                row = MSG * u + EXT + 8 * r
                m_scr[r, pl.ds(pl.multiple_of((i * GRP + u) * 8, 8), 8), :] = block[row : row + 8]
        return total

    total = lax.fori_loop(0, OWN // GRP, unpour, jnp.zeros((1, STK), F32))
    total = total[:, 0:8] + total[:, 8:16] + total[:, 16:24]
    sum_ref[...] = jnp.concatenate([total[:, 0:4], total[:, 4:8]], axis=0)
    cols = []
    for b in range(4):
        picks = [m_scr[r, pl.ds(2 * b + p, OWN, stride=8), :] for p in range(2) for r in range(DEP)]
        cols.append(jnp.concatenate(picks, axis=0))
    spectrum = jnp.concatenate(cols, axis=1).astype(BF)
    sticks = dot(zi_ref[...], spectrum).astype(BF)
    fold = N // 2
    sticks = [
        jnp.concatenate(
            [
                jnp.concatenate(
                    [sticks[p * N + q * fold : p * N + (q + 1) * fold, b * STK : (b + 1) * STK] for q in range(2)], axis=1
                )
                for b in range(4)
            ],
            axis=0,
        )
        for p in range(2)
    ]

    def pick(i, carry):
        cut = pl.ds(pl.multiple_of(i * CUT, CUT), CUT)
        hit = iota((fold, CUT), 0) == slot_ref[:, cut] >> 8
        hot = hot_ref[:, cut]
        lines = []
        for p in range(2):
            res = dot(sticks[p], hot)
            lines.append(
                [jnp.sum(jnp.where(hit, res[b * fold : (b + 1) * fold], 0.0), axis=0, keepdims=True) for b in range(4)]
            )
        for b in range(4):
            done = jnp.concatenate([lines[0][b], lines[1][b]], axis=0) + base_ref[b, :, cut]
            out_ref[b, :, cut] = done.astype(BF)
        return carry

    lax.fori_loop(0, npw // CUT, pick, 0, unroll=8)


def overlap_kernel(sub_ref, *refs):
    refs, out_refs = refs[:4], refs[4:]
    sub = sub_ref[...].astype(F32)
    sub = jnp.concatenate([sub[:, 0], sub[:, 1]], axis=1).astype(BF)
    rows = []
    for ref in refs:
        prev = ref[...].astype(F32)
        re, im = prev[:, 0], prev[:, 1]
        rows.append(jnp.concatenate([re, im], axis=1))
        rows.append(jnp.concatenate([im, -re], axis=1))
    res = dot(sub, jnp.concatenate(rows, axis=0).astype(BF), NT)
    top = res.astype(BF).astype(F32)
    mid = (res - top).astype(BF).astype(F32)
    low = res - top - mid
    pad = jnp.zeros((16, STK - 24), F32)
    for k in range(4):
        cut = slice(8 * k, 8 * (k + 1))
        out_refs[k][...] = jnp.concatenate([top[:, cut], mid[:, cut], low[:, cut], pad], axis=1).astype(BF)


def run(kernel, outs, scratch, args, near, room, to=None):
    space = [pltpu.VMEM if n else pltpu.HBM for n in near]
    return pl.pallas_call(
        kernel,
        out_shape=outs,
        in_specs=[pl.BlockSpec(memory_space=m) for m in space],
        **({} if to is None else {"out_specs": pl.BlockSpec(memory_space=to)}),
        scratch_shapes=scratch,
        compiler_params=pltpu.CompilerParams(vmem_limit_bytes=room << 20),
    )(*[pltpu.with_memory_space_constraint(a, m) for a, m in zip(args, space)])


def like(a):
    return pltpu.VMEM(a.shape, a.dtype)


def stage_pack(*args):
    args = (*args, jnp.asarray(tables()["zf"]))
    npw = args[1].shape[1]
    return run(
        pack_kernel,
        pltpu.HBM((OWN * MSG, STK), BF),
        [
            pltpu.VMEM((DEP * STK, npw), BF),
            pltpu.VMEM((512, npw), BF),
            pltpu.VMEM((DEP, OWN * 8, STK), F32),
            pltpu.VMEM((OWN * MSG, STK), BF),
            *map(like, args),
            pltpu.SemaphoreType.DMA((4 + OWN // GRP,)),
        ],
        args,
        (0, 0, 0, 0),
        24,
        pltpu.HBM,
    )


def stage_over(sub, prevs):
    return run(overlap_kernel, [pltpu.VMEM((16, STK), BF)] * 4, [], (sub, *prevs), (1, 1, 1, 1, 1), 8)


def stage_plane(got, pot):
    args = [jnp.asarray(tables()[k]) for k in ("yf", "xe", "xo", "ie", "io", "yi")]
    return run(
        plane_kernel,
        pltpu.VMEM((OWN * MSG, STK), BF),
        [
            pltpu.VMEM((OWN, W, STK), BF),
            pltpu.VMEM((OWN, STK), F32),
            pltpu.VMEM((ROWS * N, STK), F32),
            pltpu.VMEM((ROWS * N, STK), F32),
            like(pot),
            *map(like, args),
            pltpu.SemaphoreType.DMA((7,)),
        ],
        (got, pot, *args),
        (1, 0, 0, 0, 0, 0, 0, 0),
        32,
    )


def stage_ready(orb, slot, col):
    args = (orb, slot, col, jnp.asarray(tables()["zi"]))
    return run(
        ready_kernel,
        [pltpu.VMEM((W, slot.shape[1]), BF), pltpu.VMEM(orb.shape, F32), like(slot), like(args[3])],
        [like(orb), like(col), pltpu.SemaphoreType.DMA((4,))],
        args,
        (0, 0, 0, 0),
        12,
    )


def stage_wave(got, hot, base, slot, zi):
    return run(
        wave_kernel,
        (jax.ShapeDtypeStruct(base.shape, BF), jax.ShapeDtypeStruct((2, 4), F32)),
        [pltpu.VMEM((DEP, OWN * 8, STK), F32)],
        (got, hot, base, slot, zi),
        (1, 1, 1, 1, 1),
        16,
    )


def exchange(tiles):
    return lax.all_to_all(tiles, "fft", 0, 0, tiled=True).reshape(OWN * MSG, STK)


TILES = (OWN, MSG // 2, 2, STK)


def per_device(orbitals, sphere_slot, stick_column, potential, subspace, previous):
    npw = sphere_slot.shape[0]
    slot = sphere_slot.reshape(1, npw)
    col = stick_column.reshape(1, STK)

    def swapped(a, k):
        return lax.ppermute(a, "band", [(g, g ^ k) for g in range(4)])

    across = swapped(previous, 2)
    send = stage_pack(orbitals, slot, col)
    got = exchange(send.reshape(TILES))
    others = [swapped(previous, 1), across, swapped(across, 1)]
    over = stage_over(subspace, [previous, *others])
    mine = [over[0]] + [swapped(over[k], k) for k in (1, 2, 3)]
    prepared = stage_ready(orbitals, slot, col)
    field = stage_plane(got, potential)
    group = lax.axis_index("band")
    for k in (1, 2):
        mine = [jnp.where((group & k) > 0, mine[i ^ k], mine[i]) for i in range(4)]
    sums = jnp.concatenate(mine, axis=0).reshape(OWN, 1, 1, STK)
    head = jnp.pad(sums, ((0, 0), (0, 0), (0, EXT - 1), (0, 0)))
    back = exchange(lax.dynamic_update_slice(field.reshape(TILES), head, (0, 0, 0, 0)))
    applied, total = stage_wave(back, *prepared)
    return applied, total.reshape(2, 1, 4)


def solution(mesh):
    return jax.shard_map(
        per_device,
        mesh=mesh,
        in_specs=(
            P("band", None, "fft"),
            P("fft"),
            P("fft"),
            P("fft", None, None),
            P("band", None, "fft"),
            P("band", None, "fft"),
        ),
        out_specs=(P("band", None, "fft"), P(None, "fft", "band")),
        check_vma=False,
    )
```
